128 devices in a mesh: ep: 8 (over y, core), fs: 16 (over z, x).
Axes of the slice: x: 4, y: 4, z: 4, core: 2. Of those that a mesh axis runs over, the one named last changes fastest.
Arguments:
- grads: bfloat16 [8, 8, 256, 14336], P('ep', None, 'fs'), may hold values from -64 to 64
- counts: int32 [8, 8], replicated, may hold values from 16 to 2047
- weight: bfloat16 [8, 256, 14336], P('ep', 'fs'), may hold values from -3 to 3
- mom: float32 [8, 256, 14336], P('ep', 'fs'), may hold values from -64 to 64
- second: float32 [8, 256, 14336], P('ep', 'fs'), may hold values from 0.1 to 10
- in_weight: float32 [6, 32], replicated, may hold values from -2.5 to 2.5
- in_bias: float32 [32], replicated, may hold values from -3 to 3
- out_weight: float32 [32, 2], replicated, may hold values from -1 to 1
- out_bias: float32 [2], replicated, may hold values from -3 to 3
Outputs:
- new_weight: bfloat16 [8, 256, 14336], P('ep')
- new_mom: float32 [8, 256, 14336], P('ep', 'fs')
- new_second: float32 [8, 256, 14336], P('ep', 'fs')
The draws below stay inside these ranges and needn't reach their ends.
All inputs are finite; a program needn't handle non-finite values.
Results may differ from the reference program's by a relative error of at most 0.0019.
Values may be sent and summed in bfloat16 or wider, within the bound.
A program may use at most 64 MiB of HBM per device.

```python
import math
import jax
import jax.numpy as jnp
from jax import lax

FF = 14336
EXPERTS = 8
R = 256
HID = 32
FEATS = 6


def scaled_field(key, field_shape, magnitude):
    key_noise, key_cols = jax.random.split(key, 2)
    row_scale = 10.0 ** (jnp.arange(R, dtype=jnp.float32) / R)
    col_scale = jnp.exp(jax.random.uniform(key_cols, (FF,), jnp.float32, 0.0, math.log(10.0)))
    noise_field = jnp.clip(jax.random.normal(key_noise, field_shape, jnp.float32), -6.0, 6.0)
    return magnitude * noise_field * row_scale[:, None] * col_scale


def draw_grads(key, part):
    return scaled_field(jax.random.fold_in(key, 101), (EXPERTS, EXPERTS, R, FF), 0.01).astype(jnp.bfloat16)


def draw_mom(key, part):
    return scaled_field(jax.random.fold_in(key, 202), (EXPERTS, R, FF), 0.01)


def touch_ends(array, stream_key, least, top_value):
    index_at = [jax.random.randint(jax.random.fold_in(stream_key, axis), (), 0, length) for axis, length in enumerate(array.shape)]
    longest = array.shape.index(max(array.shape))
    neighbour = index_at[:longest] + [(index_at[longest] + 1) % array.shape[longest]] + index_at[longest + 1:]
    return array.at[tuple(index_at)].set(least).at[tuple(neighbour)].set(top_value)


def level_of(rng, shape, cuts, smallest, top_value):
    factor_of = 1.0
    for position, shards_of in cuts:
        draws = jax.random.uniform(jax.random.fold_in(jax.random.fold_in(rng, 6), position), (shards_of,), jnp.float32, smallest / len(cuts), top_value / len(cuts))
        factor_of = factor_of * jnp.repeat(jnp.exp(draws), shape[position] // shards_of).reshape((-1,) + (1,) * (len(shape) - 1 - position))
    return factor_of


def noise(stream_key, shape, spread, most, cuts=(), held_as=jnp.bfloat16):
    values = jax.random.normal(stream_key, shape, jnp.float32) * spread
    if len(cuts) > 0:
        values = level_of(stream_key, shape, cuts, -0.22, 0.18) * values
    return jnp.clip(values, min=-most, max=most).astype(held_as)


def setup_inputs(seed: int = 0) -> dict:
    key_list = jax.random.split(jax.random.key(seed), 10)
    return {
        "grads": draw_grads(jax.random.fold_in(key_list[9], 71), 0),
        "counts": touch_ends(jax.random.randint(key_list[1], (EXPERTS, EXPERTS), 16, 2048), jax.random.fold_in(key_list[1], 1), 16, 2047).astype(jnp.int32),
        "weight": noise(key_list[2], (EXPERTS, R, FF), 0.5, 3.0, ((0, 8), (1, 16))),
        "mom": draw_mom(jax.random.fold_in(key_list[9], 71), 0),
        "second": jnp.clip(jnp.exp(math.log(10.0) - 4.6051702 * jax.random.uniform(key_list[4], (EXPERTS, R, FF), jnp.float32) ** level_of(key_list[4], (EXPERTS, R, FF), ((0, 8), (1, 16)), -0.2, 0.2)), 0.1, 10.0),
        "in_weight": noise(key_list[5], (FEATS, HID), FEATS ** -0.5, 2.5, (), jnp.float32),
        "in_bias": noise(key_list[6], (HID,), 0.5, 3.0, (), jnp.float32),
        "out_weight": noise(key_list[7], (HID, 2), HID ** -0.5, 1.0, (), jnp.float32),
        "out_bias": noise(key_list[8], (2,), 0.5, 3.0, (), jnp.float32),
    }


MOMENTUM_DECAY = 0.9
SECOND_DECAY = 0.99
NORM_EPS = 1e-06
ROOT_EPS = 1e-08
STEP_SCALE = 0.2
EXP_SCALE = 0.5

def learned_step(gradient, mom_next, second_next, weight, grad_norm, mom_norm, in_weight, in_bias, out_weight, out_bias):
    inv_root = lax.rsqrt(second_next + ROOT_EPS)
    features = jnp.stack([gradient / grad_norm, mom_next / mom_norm, mom_next * inv_root, gradient * inv_root, weight.astype(jnp.float32), jnp.broadcast_to(jnp.log(mom_norm), gradient.shape)])
    hidden = jax.nn.relu(jnp.einsum('fh,fab->hab', in_weight, features, precision=lax.Precision.HIGHEST) + in_bias[:, None, None])
    outputs = jnp.einsum('hk,hab->kab', out_weight, hidden, precision=lax.Precision.HIGHEST) + out_bias[:, None, None]
    update = STEP_SCALE * outputs[0] * jnp.exp(EXP_SCALE * outputs[1])
    return (weight.astype(jnp.float32) - update).astype(jnp.bfloat16)

def reference(grads, counts, weight, mom, second, in_weight, in_bias, out_weight, out_bias):
    counts_f = counts.astype(jnp.float32)
    totals = lax.optimization_barrier(jnp.sum(counts_f, axis=0))
    shares = counts_f / totals[None, :]

    def per_expert(items):
        expert_grads, expert_shares, expert_weight, expert_mom, expert_second = items
        weighted = (expert_shares[:, None, None] * expert_grads.astype(jnp.float32)).astype(jnp.bfloat16)
        weighted = lax.optimization_barrier(weighted)
        gradient = lax.optimization_barrier(jnp.sum(weighted.astype(jnp.float32), axis=0))
        mom_next = MOMENTUM_DECAY * expert_mom + (1.0 - MOMENTUM_DECAY) * gradient
        second_next = SECOND_DECAY * expert_second + (1.0 - SECOND_DECAY) * gradient * gradient
        entries = gradient.shape[0] * gradient.shape[1]
        grad_norm = jnp.sqrt(jnp.sum(gradient * gradient) / entries + NORM_EPS)
        mom_norm = jnp.sqrt(jnp.sum(mom_next * mom_next) / entries + NORM_EPS)
        updated = learned_step(gradient, mom_next, second_next, expert_weight, grad_norm, mom_norm, in_weight, in_bias, out_weight, out_bias)
        return (updated, mom_next, second_next)
    new_weight, new_mom, new_second = lax.map(per_expert, (jnp.swapaxes(grads, 0, 1), shares.T, weight, mom, second))
    return (new_weight, new_mom, new_second)
```

```python
import functools

import jax
import jax.numpy as jnp
from jax import lax
from jax.experimental import pallas as pl
from jax.experimental.pallas import tpu as pltpu
from jax.sharding import PartitionSpec as P

MOMENTUM_DECAY = 0.9
SECOND_DECAY = 0.99
NORM_EPS = 1e-06
ROOT_EPS = 1e-08
STEP_SCALE = 0.2
EXP_SCALE = 0.5

ROWS = 16
LANE = 128
CHUNKS = 7
LAG = (1, 2, 3)
MESH = pl.DeviceIdType.MESH
F32 = jnp.float32
BF16 = jnp.bfloat16

CODE_POWER = 6.0
CODE_SCALE = 2.0**14


def encode(x):
    y = jnp.exp(CODE_POWER * jnp.log(jnp.abs(x) * CODE_SCALE))
    return jnp.where(x < 0, -y, y).astype(BF16)


def decode(code):
    v = code.astype(F32)
    m = jnp.exp(jnp.log(jnp.abs(v)) * (1.0 / CODE_POWER)) * (1.0 / CODE_SCALE)
    return jnp.where(v < 0, -m, m)


def loop(n, body, unroll=1):
    def step(i, carry):
        body(i)
        return carry

    lax.fori_loop(0, n, step, 0, unroll=unroll)


def kernel(
    width,
    counts,
    in_weight,
    in_bias,
    out_weight,
    out_bias,
    grads_hbm,
    weight_hbm,
    mom_hbm,
    second_hbm,
    gathered,
    new_mom,
    new_second,
    grads,
    weight,
    mom,
    second,
    to_pair,
    from_pair,
    far_out,
    far_in,
    up_out,
    up_in,
    down_out,
    down_in,
    own_sum,
    part_sum,
    shares,
    table,
    sums_out,
    sums_in,
    sums_out_z,
    sums_in_z,
    load_sem,
    pair_send,
    pair_recv,
    ring_send,
    ring_recv,
    sums_send,
    sums_recv,
    gather_send,
    gather_recv,
):
    wc = width // CHUNKS
    half = wc // 2
    quarter = wc // 4
    ep = lax.axis_index("ep")
    fs = lax.axis_index("fs")
    y, core = ep // 2, ep % 2
    z, x = fs // 4, fs % 4

    def on_y(step):
        return {"ep": ((y + step) % 4) * 2 + core}

    def on_x(step):
        return {"fs": z * 4 + (x + step) % 4}

    def on_z(step):
        return {"fs": ((z + step) % 4) * 4 + x}

    partner = {"ep": y * 2 + (1 - core)}

    def cols(k, start=0, size=None):
        return pl.ds(pl.multiple_of(k * wc + start, LANE), wc if size is None else size)

    def grads_load(k):
        return pltpu.make_async_copy(
            grads_hbm.at[0, :, :, cols(k)], grads.at[:, :, cols(k)], load_sem.at[k]
        )

    state_loads = [
        pltpu.make_async_copy(src.at[0], dst, load_sem.at[CHUNKS + i])
        for i, (src, dst) in enumerate(
            ((weight_hbm, weight), (mom_hbm, mom), (second_hbm, second))
        )
    ]
    loop(CHUNKS, lambda k: grads_load(k).start())
    for load in state_loads:
        load.start()

    barrier = pltpu.get_barrier_semaphore()
    peers = [partner, on_y(1), on_y(3)]
    peers += [on_x(1), on_x(2), on_x(3), on_z(1), on_z(2), on_z(3)]
    for peer in peers:
        pl.semaphore_signal(barrier, inc=1, device_id=peer, device_id_type=MESH)

    counted = counts[...].astype(F32)
    share_table = counted / jnp.sum(counted, axis=0, keepdims=True)
    row_id = lax.broadcasted_iota(jnp.int32, (8, 8), 0)
    col_id = lax.broadcasted_iota(jnp.int32, (8, 8), 1)
    for i in range(8):
        c = core if i >= 4 else 1 - core
        e = ((y + i) % 4) * 2 + c
        picked = jnp.where((row_id == ep) & (col_id == e), share_table, 0.0)
        one = jnp.sum(jnp.sum(picked, axis=1, keepdims=True), axis=0, keepdims=True)
        shares[i] = jnp.broadcast_to(one, (ROWS, LANE))

    for i in range(5):
        loop(32, lambda j, i=i: spread(table, j, i, in_weight[i, j]))
    for i in range(2):
        loop(32, lambda j, i=i: spread(table, j, 6 + i, out_weight[i, j]))

    pl.semaphore_wait(barrier, len(peers))

    tiles = wc // LANE
    half_tiles = half // LANE

    def tile(k, t):
        return pl.ds(pl.multiple_of(k * wc + t * LANE, LANE), LANE)

    def pair_copy(k):
        return pltpu.make_async_remote_copy(
            src_ref=to_pair.at[:, :, cols(k)],
            dst_ref=from_pair.at[:, :, cols(k)],
            send_sem=pair_send.at[k],
            recv_sem=pair_recv.at[k],
            device_id=partner,
            device_id_type=MESH,
        )

    def weigh(k):
        grads_load(k).wait()

        def body(t):
            at = tile(k, t)
            for i in range(4):
                e = ((y + i) % 4) * 2 + (1 - core)
                to_pair[i, :, at] = (grads[e, :, at].astype(F32) * shares[i]).astype(BF16)

        loop(tiles, body, unroll=4)
        pair_copy(k).start()

    loop(CHUNKS, weigh)

    def ring_copy(src, dst, kind, k, start, size, device):
        return pltpu.make_async_remote_copy(
            src_ref=src.at[:, cols(k, start, size)],
            dst_ref=dst.at[:, cols(k, start, size)],
            send_sem=ring_send.at[kind, k],
            recv_sem=ring_recv.at[kind, k],
            device_id=device,
            device_id_type=MESH,
        )

    def far_a(k):
        return ring_copy(far_out, far_in, 0, k, 0, half, on_y(1))

    def far_b(k):
        return ring_copy(far_out, far_in, 1, k, half, half, on_y(3))

    def up_a(k):
        return ring_copy(up_out, up_in, 2, k, 0, half, on_y(1))

    def up_b(k):
        return ring_copy(up_out, up_in, 3, k, half, half, on_y(1))

    def down_a(k):
        return ring_copy(down_out, down_in, 4, k, 0, half, on_y(3))

    def down_b(k):
        return ring_copy(down_out, down_in, 5, k, half, half, on_y(3))

    def pair_sum(i, at):
        e = ((y + i) % 4) * 2 + core
        mine = (grads[e, :, at].astype(F32) * shares[4 + i]).astype(BF16).astype(F32)
        return mine + from_pair[i, :, at].astype(F32)

    def sum_pairs(k):
        pair_copy(k).wait_recv()

        def far(t):
            at = tile(k, t)
            far_out[:, at] = encode(pair_sum(2, at))

        loop(tiles, far, unroll=2)
        far_a(k).start()
        far_b(k).start()

        def first(t):
            a, b = tile(k, t), tile(k, t + half_tiles)
            down_out[:, a] = encode(pair_sum(3, a))
            up_out[:, b] = encode(pair_sum(1, b))

        loop(half_tiles, first, unroll=2)
        up_b(k).start()
        down_a(k).start()

        def rest(t):
            a, b = tile(k, t), tile(k, t + half_tiles)
            part_sum[:, a] = pair_sum(1, a)
            part_sum[:, b] = pair_sum(3, b)
            own_sum[:, a] = pair_sum(0, a)
            own_sum[:, b] = pair_sum(0, b)

        loop(half_tiles, rest, unroll=2)

    loop(CHUNKS, sum_pairs)

    def pass_on(k):
        far_a(k).wait_recv()

        def up(t):
            at = tile(k, t)
            up_out[:, at] = encode(part_sum[:, at] + decode(far_in[:, at]))

        loop(half_tiles, up, unroll=2)
        up_a(k).start()
        far_b(k).wait_recv()

        def down(t):
            at = tile(k, t + half_tiles)
            down_out[:, at] = encode(part_sum[:, at] + decode(far_in[:, at]))

        loop(half_tiles, down, unroll=2)
        down_b(k).start()

    loop(CHUNKS, pass_on)

    for load in state_loads:
        load.wait()

    def moments(k, sums):
        up_a(k).wait_recv()
        up_b(k).wait_recv()
        down_a(k).wait_recv()
        down_b(k).wait_recv()

        def body(t, sums):
            grad_sq, mom_sq = sums
            at = tile(k, t)
            gradient = own_sum[:, at] + decode(up_in[:, at]) + decode(down_in[:, at])
            mom_next = MOMENTUM_DECAY * mom[:, at] + (1.0 - MOMENTUM_DECAY) * gradient
            squared = gradient * gradient
            own_sum[:, at] = gradient
            new_mom[:, at] = mom_next
            new_second[:, at] = SECOND_DECAY * second[:, at] + (1.0 - SECOND_DECAY) * squared
            return grad_sq + squared, mom_sq + mom_next * mom_next

        return lax.fori_loop(0, tiles, body, sums, unroll=2)

    zero = jnp.zeros((ROWS, LANE), F32)
    grad_sq, mom_sq = lax.fori_loop(0, CHUNKS, moments, (zero, zero))

    sums_out[0] = grad_sq[0:8] + grad_sq[8:16]
    sums_out[1] = mom_sq[0:8] + mom_sq[8:16]

    def sums_copy(src, dst, stage, i, device):
        return pltpu.make_async_remote_copy(
            src_ref=src,
            dst_ref=dst.at[i - 1],
            send_sem=sums_send.at[stage, i - 1],
            recv_sem=sums_recv.at[stage, i - 1],
            device_id=device,
            device_id_type=MESH,
        )

    for stage, (src, dst, toward) in enumerate(
        ((sums_out, sums_in, on_x), (sums_out_z, sums_in_z, on_z))
    ):
        for i in (1, 2, 3):
            sums_copy(src, dst, stage, i, toward(i)).start()
        for i in (1, 2, 3):
            sums_copy(src, dst, stage, i, toward(i)).wait_recv()
        total = src[...] + dst[0] + dst[1] + dst[2]
        if stage == 0:
            sums_out_z[...] = total

    entries = float(ROWS * width * 16)
    whole = jnp.sum(jnp.sum(total, axis=2, keepdims=True), axis=1, keepdims=True)
    grad_var = whole[0] / entries + NORM_EPS
    mom_var = whole[1] / entries + NORM_EPS
    inv_grad = jnp.broadcast_to(lax.rsqrt(grad_var), (8, LANE))
    inv_mom = jnp.broadcast_to(lax.rsqrt(mom_var), (8, LANE))
    log_mom = jnp.broadcast_to(0.5 * jnp.log(mom_var), (8, LANE))

    loop(32, lambda j: offset(table, j, in_weight[5, j], in_bias[j], log_mom))
    direction_bias = jnp.full((8, LANE), out_bias[0], F32)
    magnitude_bias = jnp.full((8, LANE), out_bias[1], F32)

    my_rows = pl.ds(pl.multiple_of(fs * ROWS, ROWS), ROWS)

    def network(k):
        def body(t):
            ats = [tile(k, 2 * t), tile(k, 2 * t + 1)]
            feats = []
            weights = []
            for at in ats:
                w16 = weight[:, at].astype(F32)
                for r in (0, 8):
                    rows = slice(r, r + 8)
                    g = own_sum[rows, at]
                    m = new_mom[rows, at]
                    inv_root = lax.rsqrt(new_second[rows, at] + ROOT_EPS)
                    w = w16[rows]
                    weights.append(w)
                    feats.append((g * inv_grad, m * inv_mom, m * inv_root, g * inv_root, w))
            direction = [direction_bias] * 4
            magnitude = [magnitude_bias] * 4
            for j in range(32):
                coef = [table[j, i] for i in range(8)]
                for v in range(4):
                    pre = coef[5]
                    for i in range(5):
                        pre = pre + coef[i] * feats[v][i]
                    hidden = jnp.maximum(pre, 0.0)
                    direction[v] = direction[v] + coef[6] * hidden
                    magnitude[v] = magnitude[v] + coef[7] * hidden
            fresh = [
                weights[v] - STEP_SCALE * direction[v] * jnp.exp(EXP_SCALE * magnitude[v])
                for v in range(4)
            ]
            for n, at in enumerate(ats):
                both = jnp.concatenate([fresh[2 * n], fresh[2 * n + 1]], axis=0)
                gathered[my_rows, at] = both.astype(BF16)

        loop(tiles // 2, body)

    FROM_X = {3: 0, 1: 1}
    FROM_Z = {3: 2, 1: 3}
    X2, Z2 = 4, 5
    THEN_Z = {3: 6, 1: 7}
    THEN_X = {3: 8, 1: 9}
    LAST_X, LAST_Z = 10, 11
    FULL, H1, H2 = (0, wc), (0, half), (half, half)
    B1, A1, A2, B2 = ((i * quarter, quarter) for i in range(4))
    A12 = (quarter, half)

    def block(dx, dz):
        return (((z + dz) % 4) * 4 + (x + dx) % 4) * ROWS

    def push(row, k, part, device, sem):
        where = gathered.at[pl.ds(pl.multiple_of(row, ROWS), ROWS), cols(k, *part)]
        pltpu.make_async_remote_copy(
            src_ref=where,
            dst_ref=where,
            send_sem=gather_send.at[0],
            recv_sem=gather_recv.at[sem, k],
            device_id=device,
            device_id_type=MESH,
        ).start()

    def arrived(sem, k, rows, size):
        where = gathered.at[pl.ds(0, rows), pl.ds(0, size)]
        pltpu.make_async_copy(where, where, gather_recv.at[sem, k]).wait()

    def send_own(k):
        row = block(0, 0)
        push(row, k, FULL, on_x(1), FROM_X[3])
        push(row, k, FULL, on_x(3), FROM_X[1])
        push(row, k, FULL, on_z(1), FROM_Z[3])
        push(row, k, FULL, on_z(3), FROM_Z[1])

    def along_z(row, k):
        push(row, k, H1, on_z(1), THEN_Z[3])
        push(row, k, H1, on_z(3), THEN_Z[1])

    def along_x(row, k):
        push(row, k, H2, on_x(1), THEN_X[3])
        push(row, k, H2, on_x(3), THEN_X[1])

    def relay_near(k):
        arrived(FROM_X[3], k, ROWS, wc)
        push(block(3, 0), k, A12, on_x(1), X2)
        along_z(block(3, 0), k)
        arrived(FROM_X[1], k, ROWS, wc)
        push(block(1, 0), k, B1, on_x(3), X2)
        push(block(1, 0), k, B2, on_x(3), X2)
        along_z(block(1, 0), k)
        arrived(FROM_Z[3], k, ROWS, wc)
        push(block(0, 3), k, A12, on_z(1), Z2)
        along_x(block(0, 3), k)
        arrived(FROM_Z[1], k, ROWS, wc)
        push(block(0, 1), k, B1, on_z(3), Z2)
        push(block(0, 1), k, B2, on_z(3), Z2)
        along_x(block(0, 1), k)

    def relay_far(k):
        arrived(X2, k, ROWS, wc)
        along_z(block(2, 0), k)
        arrived(Z2, k, ROWS, wc)
        along_x(block(0, 2), k)

    def relay_last(k):
        arrived(THEN_Z[3], k, 3 * ROWS, half)
        for i in (1, 2, 3):
            push(block(i, 3), k, A1, on_z(1), LAST_Z)
        arrived(THEN_Z[1], k, 3 * ROWS, half)
        for i in (1, 2, 3):
            push(block(i, 1), k, B1, on_z(3), LAST_Z)
        arrived(THEN_X[3], k, 3 * ROWS, half)
        for i in (1, 2, 3):
            push(block(3, i), k, A2, on_x(1), LAST_X)
        arrived(THEN_X[1], k, 3 * ROWS, half)
        for i in (1, 2, 3):
            push(block(1, i), k, B2, on_x(3), LAST_X)

    def step(t):
        @pl.when(t < CHUNKS)
        def _():
            network(t)
            send_own(t)

        for lag, relay in zip(LAG, (relay_near, relay_far, relay_last)):

            @pl.when((t >= lag) & (t < CHUNKS + lag))
            def _(lag=lag, relay=relay):
                relay(t - lag)

    loop(CHUNKS + LAG[-1], step)

    def drain(k):
        arrived(LAST_X, k, 3 * ROWS, half)
        arrived(LAST_Z, k, 3 * ROWS, half)
        pair_copy(k).wait_send()
        for copy in (far_a, far_b, up_a, up_b, down_a, down_b):
            copy(k).wait_send()

    loop(CHUNKS, drain)
    for i in (1, 2, 3):
        sums_copy(sums_out, sums_in, 0, i, on_x(i)).wait_send()
        sums_copy(sums_out_z, sums_in_z, 1, i, on_z(i)).wait_send()
    sent = gathered.at[pl.ds(0, 15 * ROWS), :]
    pltpu.make_async_copy(sent, sent, gather_send.at[0]).wait()


def spread(table, j, i, value):
    table[j, i] = jnp.full((8, LANE), value, F32)


def offset(table, j, slope, bias, log_mom):
    table[j, 5] = log_mom * slope + bias


def per_device(grads, counts, weight, mom, second, in_weight, in_bias, out_weight, out_bias):
    rows, width = mom.shape[1:]
    hbm = pl.BlockSpec(memory_space=pltpu.HBM)
    smem = pl.BlockSpec(memory_space=pltpu.SMEM)
    vmem = pl.BlockSpec(memory_space=pltpu.VMEM)
    dma = pltpu.SemaphoreType.DMA
    gathered, new_mom, new_second = pl.pallas_call(
        functools.partial(kernel, width),
        out_shape=(
            pltpu.VMEM((rows * 16, width), BF16),
            pltpu.VMEM((rows, width), F32),
            pltpu.VMEM((rows, width), F32),
        ),
        in_specs=[vmem, smem, smem, smem, smem, hbm, hbm, hbm, hbm],
        out_specs=(vmem, vmem, vmem),
        scratch_shapes=[
            pltpu.VMEM((8, rows, width), BF16),
            pltpu.VMEM((rows, width), BF16),
            pltpu.VMEM((rows, width), F32),
            pltpu.VMEM((rows, width), F32),
            pltpu.VMEM((4, rows, width), BF16),
            pltpu.VMEM((4, rows, width), BF16),
            *[pltpu.VMEM((rows, width), BF16)] * 6,
            pltpu.VMEM((rows, width), F32),
            pltpu.VMEM((rows, width), F32),
            pltpu.VMEM((8, rows, LANE), F32),
            pltpu.VMEM((32, 8, 8, LANE), F32),
            pltpu.VMEM((2, 8, LANE), F32),
            pltpu.VMEM((3, 2, 8, LANE), F32),
            pltpu.VMEM((2, 8, LANE), F32),
            pltpu.VMEM((3, 2, 8, LANE), F32),
            dma((CHUNKS + 3,)),
            dma((CHUNKS,)),
            dma((CHUNKS,)),
            dma((6, CHUNKS)),
            dma((6, CHUNKS)),
            dma((2, 3)),
            dma((2, 3)),
            dma((1,)),
            dma((12, CHUNKS)),
        ],
        compiler_params=pltpu.CompilerParams(
            collective_id=0, has_side_effects=True, vmem_limit_bytes=36 << 20
        ),
        name="learned_step",
    )(counts, in_weight, in_bias, out_weight.T, out_bias, grads, weight, mom, second)
    return gathered[None], new_mom[None], new_second[None]


def solution(mesh):
    in_specs = (
        P("ep", None, "fs", None),
        P(),
        P("ep", "fs", None),
        P("ep", "fs", None),
        P("ep", "fs", None),
        P(),
        P(),
        P(),
        P(),
    )
    out_specs = (P("ep", None, None), P("ep", "fs", None), P("ep", "fs", None))
    return jax.shard_map(
        per_device, mesh=mesh, in_specs=in_specs, out_specs=out_specs, check_vma=False
    )
```

```python
import functools

import jax
import jax.numpy as jnp
from jax import lax
from jax.experimental import pallas as pl
from jax.experimental.pallas import tpu as pltpu
from jax.sharding import PartitionSpec as P

MOMENTUM_DECAY = 0.9
SECOND_DECAY = 0.99
NORM_EPS = 1e-06
ROOT_EPS = 1e-08
STEP_SCALE = 0.2
EXP_SCALE = 0.5

ROWS = 16
LANE = 128
PARTS = 8
CHUNKS = 14
LAG = (3, 7, 14)
OTHERS = sorted(
    ((dx, dz) for dz in range(4) for dx in range(4) if dx or dz),
    key=lambda d: -min(d[0], 4 - d[0]) - min(d[1], 4 - d[1]),
)
STEPS = (2, 1, 3, 0)
MESH = pl.DeviceIdType.MESH
F32 = jnp.float32
BF16 = jnp.bfloat16

CODE_POWER = 6.0
CODE_SCALE = 2.0**14


def encode(x):
    y = jnp.exp(CODE_POWER * jnp.log(jnp.abs(x) * CODE_SCALE))
    return jnp.where(x < 0, -y, y).astype(BF16)


def decode(code):
    v = code.astype(F32)
    m = jnp.exp(jnp.log(jnp.abs(v)) * (1.0 / CODE_POWER)) * (1.0 / CODE_SCALE)
    return jnp.where(v < 0, -m, m)


def loop(n, body, unroll=1):
    def step(i, carry):
        body(i)
        return carry

    lax.fori_loop(0, n, step, 0, unroll=unroll)


def kernel(
    width,
    counts_hbm,
    in_weight_hbm,
    in_bias_hbm,
    out_weight_hbm,
    out_bias_hbm,
    grads_hbm,
    weight_hbm,
    mom_hbm,
    second_hbm,
    gathered,
    new_mom,
    new_second,
    counts,
    in_weight,
    in_bias,
    out_weight,
    out_bias,
    grads,
    weight,
    mom,
    second,
    to_pair,
    from_pair,
    far_out,
    far_in,
    up_out,
    up_in,
    down_out,
    down_in,
    own_sum,
    part_sum,
    shares,
    table,
    matrix,
    matrix_tail,
    hidden_a,
    hidden_b,
    sums_out,
    sums_in,
    load_sem,
    early_send,
    pair_recv,
    ring_recv,
    sums_sem,
    gather_send,
    gather_recv,
    last_recv,
):
    wc = width // CHUNKS
    half = wc // 2
    quarter = wc // 4
    ep = lax.axis_index("ep")
    fs = lax.axis_index("fs")
    y, core = ep // 2, ep % 2
    z, x = fs // 4, fs % 4

    def on_y(step):
        return {"ep": ((y + step) % 4) * 2 + core}

    def on_x(step):
        return {"fs": z * 4 + (x + step) % 4}

    def on_z(step):
        return {"fs": ((z + step) % 4) * 4 + x}

    partner = {"ep": y * 2 + (1 - core)}

    def await_bytes(sem, rows, size):
        where = gathered.at[pl.ds(0, rows), pl.ds(0, size)]
        pltpu.make_async_copy(where, where, sem).wait()

    def await_rows(sem, rows):
        await_bytes(sem, rows, width)

    def cols(k, start=0, size=None):
        return pl.ds(pl.multiple_of(k * wc + start, LANE), wc if size is None else size)

    def grads_load(k):
        return pltpu.make_async_copy(
            grads_hbm.at[0, :, :, cols(k)], grads.at[:, :, cols(k)], load_sem.at[k]
        )

    state_loads = [
        pltpu.make_async_copy(src.at[0], dst, load_sem.at[CHUNKS])
        for src, dst in ((weight_hbm, weight), (mom_hbm, mom), (second_hbm, second))
    ]
    barrier = pltpu.get_barrier_semaphore()
    peers = [partner, on_y(1), on_y(3)]
    peers += [{"fs": ((z + dz) % 4) * 4 + (x + dx) % 4} for dx, dz in OTHERS]
    for peer in peers:
        pl.semaphore_signal(barrier, inc=1, device_id=peer, device_id_type=MESH)

    small_loads = [
        pltpu.make_async_copy(src, dst, load_sem.at[CHUNKS + 1 + i])
        for i, (src, dst) in enumerate(
            (
                (counts_hbm, counts),
                (in_weight_hbm, in_weight),
                (in_bias_hbm, in_bias),
                (out_weight_hbm, out_weight),
                (out_bias_hbm, out_bias),
            )
        )
    ]
    small_loads[0].start()
    loop(CHUNKS, lambda k: grads_load(k).start())
    for load in small_loads[1:] + state_loads:
        load.start()

    small_loads[0].wait()
    counted = counts[...].astype(F32)
    share_table = counted / jnp.sum(counted, axis=0, keepdims=True)
    row_id = lax.broadcasted_iota(jnp.int32, (8, 8), 0)
    col_id = lax.broadcasted_iota(jnp.int32, (8, 8), 1)
    for i in range(8):
        c = core if i >= 4 else 1 - core
        e = ((y + STEPS[i % 4]) % 4) * 2 + c
        picked = jnp.where((row_id == ep) & (col_id == e), share_table, 0.0)
        one = jnp.sum(jnp.sum(picked, axis=1, keepdims=True), axis=0, keepdims=True)
        shares[i] = jnp.broadcast_to(one, (ROWS, LANE))

    with jax.named_scope("barrier"):
        pl.semaphore_wait(barrier, len(peers))

    tiles = wc // LANE
    half_tiles = half // LANE

    def tile(k, t):
        return pl.ds(pl.multiple_of(k * wc + t * LANE, LANE), LANE)

    def pair_copy(part, k):
        which = pl.ds(0, 1) if part == 0 else pl.ds(1, 3)
        return pltpu.make_async_remote_copy(
            src_ref=to_pair.at[which, :, cols(k)],
            dst_ref=from_pair.at[which, :, cols(k)],
            send_sem=early_send.at[0],
            recv_sem=pair_recv.at[part, k],
            device_id=partner,
            device_id_type=MESH,
        )

    def weigh(part, k):
        if part == 0:
            grads_load(k).wait()

        def body(t):
            at = tile(k, t)
            for n in (0,) if part == 0 else (1, 2, 3):
                e = ((y + STEPS[n]) % 4) * 2 + (1 - core)
                to_pair[n, :, at] = (grads[e, :, at].astype(F32) * shares[n]).astype(BF16)

        loop(tiles, body, unroll=4)
        pair_copy(part, k).start()

    with jax.named_scope("weigh"):
        loop(CHUNKS, functools.partial(weigh, 0))
        loop(CHUNKS, functools.partial(weigh, 1))

    def ring_copy(src, dst, kind, k, start, size, device):
        return pltpu.make_async_remote_copy(
            src_ref=src.at[:, cols(k, start, size)],
            dst_ref=dst.at[:, cols(k, start, size)],
            send_sem=early_send.at[0],
            recv_sem=ring_recv.at[min(kind, 2), k],
            device_id=device,
            device_id_type=MESH,
        )

    def far_a(k):
        return ring_copy(far_out, far_in, 0, k, 0, half, on_y(1))

    def far_b(k):
        return ring_copy(far_out, far_in, 1, k, half, half, on_y(3))

    def up_a(k):
        return ring_copy(up_out, up_in, 2, k, 0, half, on_y(1))

    def up_b(k):
        return ring_copy(up_out, up_in, 3, k, half, half, on_y(1))

    def down_a(k):
        return ring_copy(down_out, down_in, 4, k, 0, half, on_y(3))

    def down_b(k):
        return ring_copy(down_out, down_in, 5, k, half, half, on_y(3))

    def pair_sum(step, at):
        n = STEPS.index(step)
        e = ((y + step) % 4) * 2 + core
        mine = (grads[e, :, at].astype(F32) * shares[4 + n]).astype(BF16).astype(F32)
        return mine + from_pair[n, :, at].astype(F32)

    def sum_far(k):
        pair_copy(0, k).wait_recv()

        def far(t):
            at = tile(k, t)
            far_out[:, at] = encode(pair_sum(2, at))

        loop(tiles, far, unroll=2)
        far_a(k).start()
        far_b(k).start()

    def sum_near(k):
        pair_copy(1, k).wait_recv()

        def first(t):
            a, b = tile(k, t), tile(k, t + half_tiles)
            down_out[:, a] = encode(pair_sum(3, a))
            up_out[:, b] = encode(pair_sum(1, b))

        loop(half_tiles, first, unroll=2)
        up_b(k).start()
        down_a(k).start()

        def rest(t):
            a, b = tile(k, t), tile(k, t + half_tiles)
            part_sum[:, a] = pair_sum(1, a)
            part_sum[:, b] = pair_sum(3, b)
            own_sum[:, a] = pair_sum(0, a)
            own_sum[:, b] = pair_sum(0, b)

        loop(half_tiles, rest, unroll=2)

    with jax.named_scope("sum_pairs"):
        loop(CHUNKS, sum_far)
        loop(CHUNKS, sum_near)

    for load in small_loads[1:]:
        load.wait()
    lane = lax.broadcasted_iota(jnp.int32, (8, 2 * LANE), 1)
    same_row = lane % 8 == lax.broadcasted_iota(jnp.int32, (8, 2 * LANE), 0)
    feature = jnp.where(lane < 192, (lane % 32) // 8, jnp.where(lane < 216, 4, 5))
    group = lane // 32
    low = (group == 2) | ((lane >= 208) & (lane < 216))
    mid = (group == 1) | (group == 4) | ((lane >= 200) & (lane < 208))

    def fill_matrix(jj):
        parts = []
        for j in (2 * jj, 2 * jj + 1):
            value = jnp.zeros((8, 2 * LANE), F32)
            for i in range(5):
                value = jnp.where((feature == i) & same_row, in_weight[i, j], value)
            a, b, c = pieces(value)
            parts.append(jnp.where(low, c, jnp.where(mid, b, a)))
        both = jnp.concatenate(parts, axis=0)
        rows = pl.ds(pl.multiple_of(16 * jj, 16), 16)
        matrix[rows, :] = both.astype(BF16)
        matrix_tail[rows, :] = both[:, LANE:]
        for n, j in enumerate((2 * jj, 2 * jj + 1)):
            for i in range(2):
                table[j, i] = jnp.full((8, LANE), out_weight[i, j], F32)

    with jax.named_scope("fill"):
        loop(16, fill_matrix)

    def pass_on(k):
        far_a(k).wait_recv()

        def up(t):
            at = tile(k, t)
            up_out[:, at] = encode(part_sum[:, at] + decode(far_in[:, at]))

        loop(half_tiles, up, unroll=2)
        up_a(k).start()
        far_b(k).wait_recv()

        def down(t):
            at = tile(k, t + half_tiles)
            down_out[:, at] = encode(part_sum[:, at] + decode(far_in[:, at]))

        loop(half_tiles, down, unroll=2)
        down_b(k).start()

    with jax.named_scope("pass_on"):
        loop(CHUNKS, pass_on)

    await_rows(load_sem.at[CHUNKS], 5 * ROWS)

    def moments(k, sums):
        await_bytes(ring_recv.at[2, k], 2 * ROWS, wc)

        def body(t, sums):
            grad_sq, mom_sq = sums
            at = tile(k, t)
            gradient = own_sum[:, at] + decode(up_in[:, at]) + decode(down_in[:, at])
            mom_next = MOMENTUM_DECAY * mom[:, at] + (1.0 - MOMENTUM_DECAY) * gradient
            squared = gradient * gradient
            own_sum[:, at] = gradient
            new_mom[:, at] = mom_next
            new_second[:, at] = SECOND_DECAY * second[:, at] + (1.0 - SECOND_DECAY) * squared
            return grad_sq + squared, mom_sq + mom_next * mom_next

        return lax.fori_loop(0, tiles, body, sums, unroll=2)

    zero = jnp.zeros((ROWS, LANE), F32)
    with jax.named_scope("moments"):
        grad_sq, mom_sq = lax.fori_loop(0, CHUNKS, moments, (zero, zero))

    grad_sq = grad_sq[0:8] + grad_sq[8:16]
    mom_sq = mom_sq[0:8] + mom_sq[8:16]
    sums_out[...] = jnp.concatenate(
        [grad_sq[0:4] + grad_sq[4:8], mom_sq[0:4] + mom_sq[4:8]], axis=0
    )

    def sums_copy(dx, dz):
        i = dz * 4 + dx - 1
        return pltpu.make_async_remote_copy(
            src_ref=sums_out,
            dst_ref=sums_in.at[i],
            send_sem=sums_sem.at[0],
            recv_sem=sums_sem.at[1],
            device_id={"fs": ((z + dz) % 4) * 4 + (x + dx) % 4},
            device_id_type=MESH,
        )

    for dx, dz in OTHERS:
        sums_copy(dx, dz).start()
    total = sums_out[...]
    pltpu.make_async_copy(sums_in, sums_in, sums_sem.at[1]).wait()
    for i in range(15):
        total = total + sums_in[i]

    entries = float(ROWS * width * 16)
    total = jnp.sum(total, axis=1, keepdims=True)
    grad_var = jnp.sum(total[0:4], axis=0, keepdims=True) / entries + NORM_EPS
    mom_var = jnp.sum(total[4:8], axis=0, keepdims=True) / entries + NORM_EPS
    inv_grad = jnp.broadcast_to(lax.rsqrt(grad_var), (8, LANE))
    inv_mom = jnp.broadcast_to(lax.rsqrt(mom_var), (8, LANE))
    log_mom = jnp.broadcast_to(0.5 * jnp.log(mom_var), (8, LANE))

    tail_lane = lax.broadcasted_iota(jnp.int32, (8, LANE), 1) + LANE

    def fill_bias(jj):
        parts = []
        for j in (2 * jj, 2 * jj + 1):
            a, b, c = pieces(log_mom * in_weight[5, j] + in_bias[j])
            bias = jnp.where(tail_lane == 216, a, jnp.where(tail_lane == 217, b, c))
            parts.append(jnp.where((tail_lane >= 216) & (tail_lane < 219), bias, 0.0))
        rows = pl.ds(pl.multiple_of(16 * jj, 16), 16)
        both = matrix_tail[rows, :] + jnp.concatenate(parts, axis=0)
        matrix[rows, LANE:] = both.astype(BF16)

    loop(16, fill_bias, unroll=2)
    inv_grad = jnp.concatenate([inv_grad, inv_grad], axis=1)
    inv_mom = jnp.concatenate([inv_mom, inv_mom], axis=1)
    ones = jnp.ones((8, 2 * LANE), F32)
    direction_bias = jnp.full((8, LANE), out_bias[0], F32)
    magnitude_bias = jnp.full((8, LANE), out_bias[1], F32)

    my_rows = pl.ds(pl.multiple_of(fs * ROWS, ROWS), ROWS)

    last_pair = width // (2 * LANE) - 1

    def pair_at(p):
        return pl.ds(pl.multiple_of(p * (2 * LANE), 2 * LANE), 2 * LANE)

    def first_layer(p, hidden):
        at = pair_at(jnp.minimum(p, last_pair))
        w16 = weight[:, at].astype(F32)
        for n in range(2):
            rows = slice(8 * n, 8 * n + 8)
            g = own_sum[rows, at]
            m = new_mom[rows, at]
            w = w16[rows]
            inv_root = lax.rsqrt(new_second[rows, at] + ROOT_EPS)
            a1, b1, c1 = pieces(jnp.concatenate([g * inv_grad, m * inv_mom], axis=0))
            a2, b2, c2 = pieces(jnp.concatenate([m * inv_root, g * inv_root], axis=0))
            ww = jnp.concatenate([w, w], axis=0)
            wo = jnp.concatenate([w, ones], axis=0)
            stack = [a1, a2, a1, a2, a1, a2, b1, b2, b1, b2, c1, c2, ww, wo, ww, wo]
            right = jnp.concatenate([a.astype(BF16) for a in stack], axis=0)
            hidden[n] = jnp.dot(matrix[...], right, preferred_element_type=F32)

    def second_layer(p, hidden):
        at = pair_at(p)
        direction = [direction_bias] * 4
        magnitude = [magnitude_bias] * 4
        for j in range(32):
            to_direction, to_magnitude = table[j, 0], table[j, 1]
            for v in range(4):
                n, half_at = v // 2, v % 2
                h = hidden[n, 8 * j : 8 * j + 8, LANE * half_at : LANE * (half_at + 1)]
                h = jnp.maximum(h, 0.0)
                direction[v] = direction[v] + to_direction * h
                magnitude[v] = magnitude[v] + to_magnitude * h
        update = [
            STEP_SCALE * direction[v] * jnp.exp(EXP_SCALE * magnitude[v]) for v in range(4)
        ]
        rows = [jnp.concatenate(update[2 * n : 2 * n + 2], axis=1) for n in range(2)]
        fresh = weight[:, at].astype(F32) - jnp.concatenate(rows, axis=0)
        gathered[my_rows, at] = fresh.astype(BF16)

    pairs = tiles // 2

    def network(k):
        def body(t):
            p = k * pairs + 2 * t
            first_layer(p + 1, hidden_b)
            second_layer(p, hidden_a)
            first_layer(p + 2, hidden_a)
            second_layer(p + 1, hidden_b)

        loop(pairs // 2, body)

    first_layer(0, hidden_a)

    ONE, TWO, THEN = 0, 1, 2
    LAST = None
    FULL, H1, H2 = (0, wc), (0, half), (half, half)
    B1, A1, A2, B2 = ((i * quarter, quarter) for i in range(4))
    A12 = (quarter, half)

    def block(dx, dz):
        return (((z + dz) % 4) * 4 + (x + dx) % 4) * ROWS

    def push(row, k, part, device, sem):
        where = gathered.at[pl.ds(pl.multiple_of(row, ROWS), ROWS), cols(k, *part)]
        pltpu.make_async_remote_copy(
            src_ref=where,
            dst_ref=where,
            send_sem=gather_send.at[0],
            recv_sem=last_recv.at[0] if sem is LAST else gather_recv.at[sem, k],
            device_id=device,
            device_id_type=MESH,
        ).start()

    def arrived(sem, k, blocks=1):
        await_bytes(gather_recv.at[sem, k], blocks * ROWS, wc)

    def send_own(k):
        row = block(0, 0)
        push(row, k, FULL, on_x(1), ONE)
        push(row, k, FULL, on_x(3), ONE)
        push(row, k, FULL, on_z(1), ONE)
        push(row, k, FULL, on_z(3), ONE)

    def along_z(row, k):
        push(row, k, H1, on_z(1), THEN)
        push(row, k, H1, on_z(3), THEN)

    def along_x(row, k):
        push(row, k, H2, on_x(1), THEN)
        push(row, k, H2, on_x(3), THEN)

    def relay_near(k):
        arrived(ONE, k, 4)
        push(block(3, 0), k, A12, on_x(1), TWO)
        along_z(block(3, 0), k)
        push(block(1, 0), k, B1, on_x(3), TWO)
        push(block(1, 0), k, B2, on_x(3), TWO)
        along_z(block(1, 0), k)
        push(block(0, 3), k, A12, on_z(1), TWO)
        along_x(block(0, 3), k)
        push(block(0, 1), k, B1, on_z(3), TWO)
        push(block(0, 1), k, B2, on_z(3), TWO)
        along_x(block(0, 1), k)

    def relay_far(k):
        arrived(TWO, k, 2)
        along_z(block(2, 0), k)
        along_x(block(0, 2), k)

    def relay_last(k):
        arrived(THEN, k, 6)
        for i in (1, 2, 3):
            push(block(i, 3), k, A1, on_z(1), LAST)
            push(block(i, 1), k, B1, on_z(3), LAST)
            push(block(3, i), k, A2, on_x(1), LAST)
            push(block(1, i), k, B2, on_x(3), LAST)

    def step(t):
        @pl.when(t < CHUNKS)
        def _():
            with jax.named_scope("network"):
                network(t)
            send_own(t)

        for lag, relay in zip(LAG, (relay_near, relay_far, relay_last)):

            @pl.when((t >= lag) & (t < CHUNKS + lag))
            def _(lag=lag, relay=relay):
                relay(t - lag)

    with jax.named_scope("gather"):
        loop(CHUNKS + LAG[-1], step)

    with jax.named_scope("drain"):
        await_rows(last_recv.at[0], 3 * ROWS)
    await_rows(early_send.at[0], 7 * ROWS)
    pltpu.make_async_copy(sums_in, sums_in, sums_sem.at[0]).wait()
    with jax.named_scope("final"):
        await_rows(gather_send.at[0], 15 * ROWS)


def pieces(x):
    a = x.astype(BF16).astype(F32)
    b = (x - a).astype(BF16).astype(F32)
    return a, b, x - a - b


def write_out(gathered, new_mom, new_second, gathered_hbm, mom_hbm, second_hbm, sem):
    rows = gathered.shape[0] // PARTS
    copies = [
        pltpu.make_async_copy(
            gathered.at[pl.ds(i * rows, rows)], gathered_hbm.at[0, pl.ds(i * rows, rows)], sem.at[i]
        )
        for i in range(PARTS)
    ]
    copies.append(pltpu.make_async_copy(new_mom, mom_hbm.at[0], sem.at[PARTS]))
    copies.append(pltpu.make_async_copy(new_second, second_hbm.at[0], sem.at[PARTS + 1]))
    for copy in copies:
        copy.start()
    for copy in copies:
        copy.wait()


def per_device(grads, counts, weight, mom, second, in_weight, in_bias, out_weight, out_bias):
    rows, width = mom.shape[1:]
    hbm = pl.BlockSpec(memory_space=pltpu.HBM)
    vmem = pl.BlockSpec(memory_space=pltpu.VMEM)
    dma = pltpu.SemaphoreType.DMA
    gathered, new_mom, new_second = pl.pallas_call(
        functools.partial(kernel, width),
        out_shape=(
            pltpu.VMEM((rows * 16, width), BF16),
            pltpu.VMEM((rows, width), F32),
            pltpu.VMEM((rows, width), F32),
        ),
        in_specs=[hbm] * 9,
        out_specs=(vmem, vmem, vmem),
        scratch_shapes=[
            pltpu.VMEM((8, 8), jnp.int32),
            pltpu.SMEM((6, 32), F32),
            pltpu.SMEM((32,), F32),
            pltpu.SMEM((2, 32), F32),
            pltpu.SMEM((2,), F32),
            pltpu.VMEM((8, rows, width), BF16),
            pltpu.VMEM((rows, width), BF16),
            pltpu.VMEM((rows, width), F32),
            pltpu.VMEM((rows, width), F32),
            pltpu.VMEM((4, rows, width), BF16),
            pltpu.VMEM((4, rows, width), BF16),
            *[pltpu.VMEM((rows, width), BF16)] * 6,
            pltpu.VMEM((rows, width), F32),
            pltpu.VMEM((rows, width), F32),
            pltpu.VMEM((8, rows, LANE), F32),
            pltpu.VMEM((32, 2, 8, LANE), F32),
            pltpu.VMEM((256, 256), BF16),
            pltpu.VMEM((256, LANE), F32),
            pltpu.VMEM((2, 256, 256), F32),
            pltpu.VMEM((2, 256, 256), F32),
            pltpu.VMEM((8, LANE), F32),
            pltpu.VMEM((15, 8, LANE), F32),
            dma((CHUNKS + 6,)),
            dma((1,)),
            dma((2, CHUNKS)),
            dma((3, CHUNKS)),
            dma((2,)),
            dma((1,)),
            dma((3, CHUNKS)),
            dma((1,)),
        ],
        compiler_params=pltpu.CompilerParams(
            collective_id=0, has_side_effects=True, vmem_limit_bytes=36 << 20
        ),
        name="learned_step",
    )(*[
        pltpu.with_memory_space_constraint(a, pltpu.HBM)
        for a in (counts, in_weight, in_bias, out_weight.T, out_bias, grads, weight, mom, second)
    ])
    return pl.pallas_call(
        write_out,
        out_shape=tuple(
            jax.ShapeDtypeStruct((1, *a.shape), a.dtype) for a in (gathered, new_mom, new_second)
        ),
        in_specs=[vmem] * 3,
        out_specs=(hbm,) * 3,
        scratch_shapes=[dma((PARTS + 2,))],
        compiler_params=pltpu.CompilerParams(vmem_limit_bytes=1 << 20),
        name="write_out",
    )(gathered, new_mom, new_second)


def solution(mesh):
    in_specs = (
        P("ep", None, "fs", None),
        P(),
        P("ep", "fs", None),
        P("ep", "fs", None),
        P("ep", "fs", None),
        P(),
        P(),
        P(),
        P(),
    )
    out_specs = (P("ep", None, None), P("ep", "fs", None), P("ep", "fs", None))
    return jax.shard_map(
        per_device, mesh=mesh, in_specs=in_specs, out_specs=out_specs, check_vma=False
    )
```

```python
import functools

import jax
import jax.numpy as jnp
from jax import lax
from jax.experimental import pallas as pl
from jax.experimental.pallas import tpu as pltpu
from jax.sharding import PartitionSpec as P

MOMENTUM_DECAY = 0.9
SECOND_DECAY = 0.99
NORM_EPS = 1e-06
ROOT_EPS = 1e-08
STEP_SCALE = 0.2
EXP_SCALE = 0.5

ROWS = 16
LANE = 128
FIRST_CORE = 1
GO_CHUNK = 13
CHUNKS = 14
LAG = (3, 7, 14)
OTHERS = sorted(
    ((dx, dz) for dz in range(4) for dx in range(4) if dx or dz),
    key=lambda d: -min(d[0], 4 - d[0]) - min(d[1], 4 - d[1]),
)
STEPS = (2, 1, 3, 0)
MESH = pl.DeviceIdType.MESH
F32 = jnp.float32
BF16 = jnp.bfloat16

CODE_POWER = 6.0
CODE_SCALE = 2.0**14


def encode(x):
    y = jnp.exp(CODE_POWER * jnp.log(jnp.abs(x) * CODE_SCALE))
    return jnp.where(x < 0, -y, y).astype(BF16)


def decode(code):
    v = code.astype(F32)
    m = jnp.exp(jnp.log(jnp.abs(v)) * (1.0 / CODE_POWER)) * (1.0 / CODE_SCALE)
    return jnp.where(v < 0, -m, m)


def loop(n, body, unroll=1):
    def step(i, carry):
        body(i)
        return carry

    lax.fori_loop(0, n, step, 0, unroll=unroll)


def kernel(
    width,
    counts_hbm,
    in_weight_hbm,
    in_bias_hbm,
    out_weight_hbm,
    out_bias_hbm,
    grads_hbm,
    weight_hbm,
    mom_hbm,
    second_hbm,
    gathered,
    new_mom,
    new_second,
    counts,
    in_weight,
    in_bias,
    out_weight,
    out_bias,
    grads,
    weight,
    mom,
    second,
    to_pair,
    from_pair,
    far_out,
    far_in,
    up_out,
    up_in,
    down_out,
    down_in,
    own_sum,
    part_sum,
    shares,
    table,
    matrix,
    matrix_tail,
    hidden_a,
    hidden_b,
    sums_out,
    sums_in,
    load_sem,
    go,
    early_send,
    pair_recv,
    ring_recv,
    sums_sem,
    gather_send,
    gather_recv,
    last_recv,
):
    wc = width // CHUNKS
    half = wc // 2
    quarter = wc // 4
    ep = lax.axis_index("ep")
    fs = lax.axis_index("fs")
    y, core = ep // 2, ep % 2
    z, x = fs // 4, fs % 4

    def on_y(step):
        return {"ep": ((y + step) % 4) * 2 + core}

    def on_x(step):
        return {"fs": z * 4 + (x + step) % 4}

    def on_z(step):
        return {"fs": ((z + step) % 4) * 4 + x}

    partner = {"ep": y * 2 + (1 - core)}

    def await_bytes(sem, rows, size):
        where = grads.at[pl.ds(0, rows // ROWS), :, pl.ds(0, size)]
        pltpu.make_async_copy(where, where, sem).wait()


    def cols(k, start=0, size=None):
        return pl.ds(pl.multiple_of(k * wc + start, LANE), wc if size is None else size)

    def grads_load(n):
        pair = pl.ds(((y + STEPS[n]) % 4) * 2, 2)
        return pltpu.make_async_copy(grads_hbm.at[0, pair], grads.at[pair], load_sem.at[n])

    state_loads = [
        pltpu.make_async_copy(src.at[0], dst, load_sem.at[4])
        for src, dst in ((weight_hbm, weight), (mom_hbm, mom), (second_hbm, second))
    ]
    barrier = pltpu.get_barrier_semaphore()
    peers = [partner, on_y(1), on_y(3)]
    peers += [{"fs": ((z + dz) % 4) * 4 + (x + dx) % 4} for dx, dz in OTHERS]
    for peer in peers:
        pl.semaphore_signal(barrier, inc=1, device_id=peer, device_id_type=MESH)

    small_loads = [
        pltpu.make_async_copy(src, dst, load_sem.at[5 + i])
        for i, (src, dst) in enumerate(
            (
                (counts_hbm, counts),
                (in_weight_hbm, in_weight),
                (in_bias_hbm, in_bias),
                (out_weight_hbm, out_weight),
                (out_bias_hbm, out_bias),
            )
        )
    ]
    small_loads[0].start()
    for n in range(4):
        grads_load(n).start()

    small_loads[0].wait()
    counted = counts[...].astype(F32)
    share_table = counted / jnp.sum(counted, axis=0, keepdims=True)
    row_id = lax.broadcasted_iota(jnp.int32, (8, 8), 0)
    col_id = lax.broadcasted_iota(jnp.int32, (8, 8), 1)
    for i in range(8):
        c = core if i >= 4 else 1 - core
        e = ((y + STEPS[i % 4]) % 4) * 2 + c
        picked = jnp.where((row_id == ep) & (col_id == e), share_table, 0.0)
        one = jnp.sum(jnp.sum(picked, axis=1, keepdims=True), axis=0, keepdims=True)
        shares[i] = jnp.broadcast_to(one, (ROWS, LANE))

    with jax.named_scope("barrier"):
        pl.semaphore_wait(barrier, len(peers))

    tiles = wc // LANE
    half_tiles = half // LANE

    def tile(k, t):
        return pl.ds(pl.multiple_of(k * wc + t * LANE, LANE), LANE)

    def pair_copy(part, k):
        which = pl.ds(0, 1) if part == 0 else pl.ds(1, 3)
        return pltpu.make_async_remote_copy(
            src_ref=to_pair.at[which, :, cols(k)],
            dst_ref=from_pair.at[which, :, cols(k)],
            send_sem=early_send.at[0],
            recv_sem=pair_recv.at[k if part == 0 else CHUNKS],
            device_id=partner,
            device_id_type=MESH,
        )

    def weigh(part, k):
        def body(t):
            at = tile(k, t)
            for n in (0,) if part == 0 else (1, 2, 3):
                e = ((y + STEPS[n]) % 4) * 2 + (1 - core)
                to_pair[n, :, at] = (grads[e, :, at].astype(F32) * shares[n]).astype(BF16)

        loop(tiles, body, unroll=4)
        pair_copy(part, k).start()

    with jax.named_scope("weigh"):
        grads_load(0).wait()
        loop(CHUNKS, functools.partial(weigh, 0))

    def ring_copy(src, dst, kind, k, start, size, device):
        return pltpu.make_async_remote_copy(
            src_ref=src.at[:, cols(k, start, size)],
            dst_ref=dst.at[:, cols(k, start, size)],
            send_sem=early_send.at[0],
            recv_sem=ring_recv.at[kind // 2 if kind < 2 else 1, k],
            device_id=device,
            device_id_type=MESH,
        )

    def far_a(k):
        return ring_copy(far_out, far_in, 0, k, 0, half, on_y(1))

    def far_b(k):
        return ring_copy(far_out, far_in, 1, k, half, half, on_y(3))

    def up_a(k):
        return ring_copy(up_out, up_in, 2, k, 0, half, on_y(1))

    def up_b(k):
        return ring_copy(up_out, up_in, 3, k, half, half, on_y(1))

    def down_a(k):
        return ring_copy(down_out, down_in, 4, k, 0, half, on_y(3))

    def down_b(k):
        return ring_copy(down_out, down_in, 5, k, half, half, on_y(3))

    def pair_sum(step, at):
        n = STEPS.index(step)
        e = ((y + step) % 4) * 2 + core
        mine = (grads[e, :, at].astype(F32) * shares[4 + n]).astype(BF16).astype(F32)
        return mine + from_pair[n, :, at].astype(F32)

    def sum_far(k):
        pair_copy(0, k).wait_recv()

        def far(t):
            at = tile(k, t)
            far_out[:, at] = encode(pair_sum(2, at))

        loop(tiles, far, unroll=2)
        far_a(k).start()
        far_b(k).start()

    def sum_near(k):
        def first(t):
            a, b = tile(k, t), tile(k, t + half_tiles)
            down_out[:, a] = encode(pair_sum(3, a))
            up_out[:, b] = encode(pair_sum(1, b))

        loop(half_tiles, first, unroll=2)
        up_b(k).start()
        down_a(k).start()

        def rest(t):
            a, b = tile(k, t), tile(k, t + half_tiles)
            part_sum[:, a] = pair_sum(1, a)
            part_sum[:, b] = pair_sum(3, b)
            own_sum[:, a] = pair_sum(0, a)
            own_sum[:, b] = pair_sum(0, b)

        loop(half_tiles, rest, unroll=2)

    with jax.named_scope("sum_pairs"):
        @pl.when(core == FIRST_CORE)
        def _():
            loop(CHUNKS, sum_far)

        for n in (1, 2, 3):
            grads_load(n).wait()
        for load in small_loads[1:] + state_loads:
            load.start()
        loop(CHUNKS, functools.partial(weigh, 1))

        @pl.when(core != FIRST_CORE)
        def _():
            pl.semaphore_wait(go, 1)
            loop(CHUNKS, sum_far)

        pair_near = from_pair.at[pl.ds(1, 3)]
        pltpu.make_async_copy(pair_near, pair_near, pair_recv.at[CHUNKS]).wait()
        loop(CHUNKS, sum_near)

    for load in small_loads[1:]:
        load.wait()
    lane = lax.broadcasted_iota(jnp.int32, (8, 2 * LANE), 1)
    same_row = lane % 8 == lax.broadcasted_iota(jnp.int32, (8, 2 * LANE), 0)
    feature = jnp.where(lane < 192, (lane % 32) // 8, jnp.where(lane < 216, 4, 5))
    group = lane // 32
    low = (group == 2) | ((lane >= 208) & (lane < 216))
    mid = (group == 1) | (group == 4) | ((lane >= 200) & (lane < 208))

    def fill_matrix(jj):
        parts = []
        for j in (2 * jj, 2 * jj + 1):
            value = jnp.zeros((8, 2 * LANE), F32)
            for i in range(5):
                value = jnp.where((feature == i) & same_row, in_weight[i, j], value)
            a, b, c = pieces(value)
            parts.append(jnp.where(low, c, jnp.where(mid, b, a)))
        both = jnp.concatenate(parts, axis=0)
        rows = pl.ds(pl.multiple_of(16 * jj, 16), 16)
        matrix[rows, :] = both.astype(BF16)
        matrix_tail[rows, :] = both[:, LANE:]
        for n, j in enumerate((2 * jj, 2 * jj + 1)):
            for i in range(2):
                table[j, i] = jnp.full((8, LANE), out_weight[i, j], F32)

    with jax.named_scope("fill"):
        loop(16, fill_matrix)

    def pass_on(k):
        @pl.when((core == FIRST_CORE) & (k == GO_CHUNK))
        def _():
            pl.semaphore_signal(go, inc=1, device_id=partner, device_id_type=MESH)

        await_bytes(ring_recv.at[0, k], ROWS, wc)

        def up(t):
            at = tile(k, t)
            up_out[:, at] = encode(part_sum[:, at] + decode(far_in[:, at]))

        loop(half_tiles, up, unroll=2)
        up_a(k).start()

        def down(t):
            at = tile(k, t + half_tiles)
            down_out[:, at] = encode(part_sum[:, at] + decode(far_in[:, at]))

        loop(half_tiles, down, unroll=2)
        down_b(k).start()

    with jax.named_scope("pass_on"):
        loop(CHUNKS, pass_on)

    await_bytes(load_sem.at[4], 5 * ROWS, width)

    def moments(k, sums):
        await_bytes(ring_recv.at[1, k], 2 * ROWS, wc)

        def body(t, sums):
            grad_sq, mom_sq = sums
            at = tile(k, t)
            gradient = own_sum[:, at] + decode(up_in[:, at]) + decode(down_in[:, at])
            mom_next = MOMENTUM_DECAY * mom[:, at] + (1.0 - MOMENTUM_DECAY) * gradient
            squared = gradient * gradient
            own_sum[:, at] = gradient
            new_mom[:, at] = mom_next
            new_second[:, at] = SECOND_DECAY * second[:, at] + (1.0 - SECOND_DECAY) * squared
            return grad_sq + squared, mom_sq + mom_next * mom_next

        return lax.fori_loop(0, tiles, body, sums, unroll=2)

    zero = jnp.zeros((ROWS, LANE), F32)
    with jax.named_scope("moments"):
        grad_sq, mom_sq = lax.fori_loop(0, CHUNKS, moments, (zero, zero))

    sums_out[...] = jnp.concatenate(
        [jnp.sum(grad_sq, axis=0, keepdims=True), jnp.sum(mom_sq, axis=0, keepdims=True)], axis=0
    )
    sums_in[fs] = sums_out[...]

    def sums_copy(dx, dz):
        return pltpu.make_async_remote_copy(
            src_ref=sums_out,
            dst_ref=sums_in.at[fs],
            send_sem=sums_sem.at[0],
            recv_sem=sums_sem.at[1],
            device_id={"fs": ((z + dz) % 4) * 4 + (x + dx) % 4},
            device_id_type=MESH,
        )

    for dx, dz in OTHERS:
        sums_copy(dx, dz).start()
    fifteen = sums_in.at[pl.ds(0, 15)]
    with jax.named_scope("sums"):
        pltpu.make_async_copy(fifteen, fifteen, sums_sem.at[1]).wait()
    total = sums_in[0]
    for i in range(1, 16):
        total = total + sums_in[i]

    entries = float(ROWS * width * 16)
    total = jnp.sum(total, axis=1, keepdims=True)
    grad_var = total[0:1] / entries + NORM_EPS
    mom_var = total[1:2] / entries + NORM_EPS
    inv_grad = jnp.broadcast_to(lax.rsqrt(grad_var), (8, LANE))
    inv_mom = jnp.broadcast_to(lax.rsqrt(mom_var), (8, LANE))
    log_mom = jnp.broadcast_to(0.5 * jnp.log(mom_var), (8, LANE))

    tail_lane = lax.broadcasted_iota(jnp.int32, (8, LANE), 1) + LANE

    def fill_bias(jj):
        parts = []
        for j in (2 * jj, 2 * jj + 1):
            a, b, c = pieces(log_mom * in_weight[5, j] + in_bias[j])
            bias = jnp.where(tail_lane == 216, a, jnp.where(tail_lane == 217, b, c))
            parts.append(jnp.where((tail_lane >= 216) & (tail_lane < 219), bias, 0.0))
        rows = pl.ds(pl.multiple_of(16 * jj, 16), 16)
        both = matrix_tail[rows, :] + jnp.concatenate(parts, axis=0)
        matrix[rows, LANE:] = both.astype(BF16)

    loop(16, fill_bias, unroll=2)
    inv_grad = jnp.concatenate([inv_grad, inv_grad], axis=1)
    inv_mom = jnp.concatenate([inv_mom, inv_mom], axis=1)
    ones = jnp.ones((8, 2 * LANE), F32)
    direction_bias = jnp.full((8, LANE), out_bias[0], F32)
    magnitude_bias = jnp.full((8, LANE), out_bias[1], F32)


    last_pair = width // (2 * LANE) - 1

    def pair_at(p):
        return pl.ds(pl.multiple_of(p * (2 * LANE), 2 * LANE), 2 * LANE)

    def first_layer(p, hidden):
        at = pair_at(jnp.minimum(p, last_pair))
        w16 = weight[:, at].astype(F32)
        for n in range(2):
            rows = slice(8 * n, 8 * n + 8)
            g = own_sum[rows, at]
            m = new_mom[rows, at]
            w = w16[rows]
            inv_root = lax.rsqrt(new_second[rows, at] + ROOT_EPS)
            a1, b1, c1 = pieces(jnp.concatenate([g * inv_grad, m * inv_mom], axis=0))
            a2, b2, c2 = pieces(jnp.concatenate([m * inv_root, g * inv_root], axis=0))
            ww = jnp.concatenate([w, w], axis=0)
            wo = jnp.concatenate([w, ones], axis=0)
            stack = [a1, a2, a1, a2, a1, a2, b1, b2, b1, b2, c1, c2, ww, wo, ww, wo]
            right = jnp.concatenate([a.astype(BF16) for a in stack], axis=0)
            hidden[n] = jnp.dot(matrix[...], right, preferred_element_type=F32)

    def second_layer(p, hidden):
        at = pair_at(p)
        direction = [direction_bias] * 4
        magnitude = [magnitude_bias] * 4
        for j in range(32):
            to_direction, to_magnitude = table[j, 0], table[j, 1]
            for v in range(4):
                n, half_at = v // 2, v % 2
                h = hidden[n, 8 * j : 8 * j + 8, LANE * half_at : LANE * (half_at + 1)]
                h = jnp.maximum(h, 0.0)
                direction[v] = direction[v] + to_direction * h
                magnitude[v] = magnitude[v] + to_magnitude * h
        update = [
            STEP_SCALE * direction[v] * jnp.exp(EXP_SCALE * magnitude[v]) for v in range(4)
        ]
        rows = [jnp.concatenate(update[2 * n : 2 * n + 2], axis=1) for n in range(2)]
        fresh = weight[:, at].astype(F32) - jnp.concatenate(rows, axis=0)
        gathered[z, x, :, at] = fresh.astype(BF16)

    pairs = tiles // 2

    def network(k):
        def body(t):
            p = k * pairs + 2 * t
            first_layer(p + 1, hidden_b)
            second_layer(p, hidden_a)
            first_layer(p + 2, hidden_a)
            second_layer(p + 1, hidden_b)

        loop(pairs // 2, body)

    first_layer(0, hidden_a)

    ONE, TWO, THEN = 0, 1, 2
    LAST = None
    FULL, H1, H2 = (0, wc), (0, half), (half, half)
    B1, A1, A2, B2 = ((i * quarter, quarter) for i in range(4))

    def push(dx, dz, k, part, device, sem):
        at = cols(k, *part)
        if dx is None:
            where = gathered.at[(z + dz) % 4, :, :, at]
        elif dz is None:
            where = gathered.at[:, (x + dx) % 4, :, at]
        else:
            where = gathered.at[(z + dz) % 4, (x + dx) % 4, :, at]
        pltpu.make_async_remote_copy(
            src_ref=where,
            dst_ref=where,
            send_sem=gather_send.at[1 if part == FULL or sem == TWO or 2 in (dx, dz) else 0],
            recv_sem=last_recv.at[0] if sem is LAST else gather_recv.at[sem, k],
            device_id=device,
            device_id_type=MESH,
        ).start()

    def arrived(sem, k, blocks=1):
        await_bytes(gather_recv.at[sem, k], blocks * ROWS, wc)

    def send_own(k):
        for toward in (1, 3):
            push(0, 0, k, FULL, on_x(toward), ONE)
            push(0, 0, k, FULL, on_z(toward), ONE)

    def along_z(dx, dz, k):
        push(dx, dz, k, H1, on_z(1), THEN)
        push(dx, dz, k, H1, on_z(3), THEN)

    def along_x(dx, dz, k):
        push(dx, dz, k, H2, on_x(1), THEN)
        push(dx, dz, k, H2, on_x(3), THEN)

    def relay_near(k):
        arrived(ONE, k, 4)
        push(3, 0, k, A1, on_x(1), TWO)
        push(1, 0, k, B1, on_x(3), TWO)
        push(0, 3, k, A2, on_z(1), TWO)
        push(0, 1, k, B2, on_z(3), TWO)
        for d in (3, 1):
            along_z(d, 0, k)
            along_x(0, d, k)

    def relay_far(k):
        arrived(TWO, k)
        along_z(2, 0, k)
        along_x(0, 2, k)

    def relay_last(k):
        arrived(THEN, k, 6)
        push(None, 3, k, A1, on_z(1), LAST)
        push(None, 1, k, B1, on_z(3), LAST)
        push(3, None, k, A2, on_x(1), LAST)
        push(1, None, k, B2, on_x(3), LAST)

    def step(t):
        @pl.when(t < CHUNKS)
        def _():
            with jax.named_scope("network"):
                network(t)
            send_own(t)

        for lag, relay in zip(LAG, (relay_near, relay_far, relay_last)):

            @pl.when((t >= lag) & (t < CHUNKS + lag))
            def _(lag=lag, relay=relay):
                relay(t - lag)

    with jax.named_scope("gather"):
        loop(CHUNKS + LAG[-1], step)

    with jax.named_scope("drain"):
        await_bytes(last_recv.at[0], 4 * ROWS, width)
    await_bytes(early_send.at[0], 7 * ROWS, width)
    pltpu.make_async_copy(fifteen, fifteen, sums_sem.at[0]).wait()
    with jax.named_scope("final"):
        await_bytes(gather_send.at[0], 8 * ROWS, width)
        await_bytes(gather_send.at[1], 7 * ROWS, width)


def pieces(x):
    a = x.astype(BF16).astype(F32)
    b = (x - a).astype(BF16).astype(F32)
    return a, b, x - a - b


def write_out(gathered, new_mom, new_second, gathered_hbm, mom_hbm, second_hbm, sem):
    copies = [
        pltpu.make_async_copy(
            gathered.at[i // 4, i % 4], gathered_hbm.at[0, pl.ds(i * ROWS, ROWS)], sem.at[i]
        )
        for i in range(16)
    ]
    copies.append(pltpu.make_async_copy(new_mom, mom_hbm.at[0], sem.at[16]))
    copies.append(pltpu.make_async_copy(new_second, second_hbm.at[0], sem.at[17]))
    for copy in copies:
        copy.start()
    for copy in copies:
        copy.wait()


def per_device(grads, counts, weight, mom, second, in_weight, in_bias, out_weight, out_bias):
    rows, width = mom.shape[1:]
    hbm = pl.BlockSpec(memory_space=pltpu.HBM)
    vmem = pl.BlockSpec(memory_space=pltpu.VMEM)
    dma = pltpu.SemaphoreType.DMA
    gathered, new_mom, new_second = pl.pallas_call(
        functools.partial(kernel, width),
        out_shape=(
            pltpu.VMEM((4, 4, rows, width), BF16),
            pltpu.VMEM((rows, width), F32),
            pltpu.VMEM((rows, width), F32),
        ),
        in_specs=[hbm] * 9,
        out_specs=(vmem, vmem, vmem),
        scratch_shapes=[
            pltpu.VMEM((8, 8), jnp.int32),
            pltpu.SMEM((6, 32), F32),
            pltpu.SMEM((32,), F32),
            pltpu.SMEM((2, 32), F32),
            pltpu.SMEM((2,), F32),
            pltpu.VMEM((8, rows, width), BF16),
            pltpu.VMEM((rows, width), BF16),
            pltpu.VMEM((rows, width), F32),
            pltpu.VMEM((rows, width), F32),
            pltpu.VMEM((4, rows, width), BF16),
            pltpu.VMEM((4, rows, width), BF16),
            *[pltpu.VMEM((rows, width), BF16)] * 6,
            pltpu.VMEM((rows, width), F32),
            pltpu.VMEM((rows, width), F32),
            pltpu.VMEM((8, rows, LANE), F32),
            pltpu.VMEM((32, 2, 8, LANE), F32),
            pltpu.VMEM((256, 256), BF16),
            pltpu.VMEM((256, LANE), F32),
            pltpu.VMEM((2, 256, 256), F32),
            pltpu.VMEM((2, 256, 256), F32),
            pltpu.VMEM((2, LANE), F32),
            pltpu.VMEM((16, 2, LANE), F32),
            dma((10,)),
            pltpu.SemaphoreType.REGULAR,
            dma((1,)),
            dma((CHUNKS + 1,)),
            dma((2, CHUNKS)),
            dma((2,)),
            dma((2,)),
            dma((3, CHUNKS)),
            dma((1,)),
        ],
        compiler_params=pltpu.CompilerParams(
            collective_id=0, has_side_effects=True, vmem_limit_bytes=36 << 20
        ),
        name="learned_step",
    )(*[
        pltpu.with_memory_space_constraint(a, pltpu.HBM)
        for a in (counts, in_weight, in_bias, out_weight.T, out_bias, grads, weight, mom, second)
    ])
    return pl.pallas_call(
        write_out,
        out_shape=tuple(
            jax.ShapeDtypeStruct(shape, dtype)
            for shape, dtype in (
                ((1, 16 * rows, width), BF16),
                ((1, rows, width), F32),
                ((1, rows, width), F32),
            )
        ),
        in_specs=[vmem] * 3,
        out_specs=(hbm,) * 3,
        scratch_shapes=[dma((18,))],
        compiler_params=pltpu.CompilerParams(vmem_limit_bytes=1 << 20),
        name="write_out",
    )(gathered, new_mom, new_second)


def solution(mesh):
    in_specs = (
        P("ep", None, "fs", None),
        P(),
        P("ep", "fs", None),
        P("ep", "fs", None),
        P("ep", "fs", None),
        P(),
        P(),
        P(),
        P(),
    )
    out_specs = (P("ep", None, None), P("ep", "fs", None), P("ep", "fs", None))
    return jax.shard_map(
        per_device, mesh=mesh, in_specs=in_specs, out_specs=out_specs, check_vma=False
    )
```

```python
import functools

import jax
import jax.numpy as jnp
from jax import lax
from jax.experimental import pallas as pl
from jax.experimental.pallas import tpu as pltpu
from jax.sharding import PartitionSpec as P

MOMENTUM_DECAY = 0.9
SECOND_DECAY = 0.99
NORM_EPS = 1e-06
ROOT_EPS = 1e-08
STEP_SCALE = 0.2
EXP_SCALE = 0.5

ROWS = 16
LANE = 128
FIRST_CORE = 1
HEAD = 7
GO_CHUNK = 13
CHUNKS = 14
LAG = (3, 8, 14)
OTHERS = sorted(
    ((dx, dz) for dz in range(4) for dx in range(4) if dx or dz),
    key=lambda d: -min(d[0], 4 - d[0]) - min(d[1], 4 - d[1]),
)
STEPS = (2, 1, 3, 0)
MESH = pl.DeviceIdType.MESH
F32 = jnp.float32
BF16 = jnp.bfloat16

CODE_POWER = 6.0
CODE_SCALE = 2.0**14


def encode(x):
    y = jnp.exp(CODE_POWER * jnp.log(jnp.abs(x) * CODE_SCALE))
    return jnp.where(x < 0, -y, y).astype(BF16)


def decode(code):
    v = code.astype(F32)
    m = jnp.exp(jnp.log(jnp.abs(v)) * (1.0 / CODE_POWER)) * (1.0 / CODE_SCALE)
    return jnp.where(v < 0, -m, m)


def loop(n, body, unroll=1):
    def step(i, carry):
        body(i)
        return carry

    lax.fori_loop(0, n, step, 0, unroll=unroll)


def kernel(
    width,
    counts_hbm,
    in_weight_hbm,
    in_bias_hbm,
    out_weight_hbm,
    out_bias_hbm,
    grads_hbm,
    weight_hbm,
    mom_hbm,
    second_hbm,
    gathered,
    new_mom,
    new_second,
    counts,
    in_weight,
    in_bias,
    out_weight,
    out_bias,
    grads,
    weight,
    mom,
    second,
    to_pair,
    from_pair,
    far_out,
    far_in,
    up_out,
    up_in,
    down_out,
    down_in,
    own_sum,
    part_sum,
    shares,
    table,
    matrix,
    base,
    right,
    hidden_a,
    hidden_b,
    sums_out,
    sums_in,
    load_sem,
    go,
    early_send,
    pair_recv,
    ring_recv,
    sums_sem,
    gather_send,
    gather_recv,
    last_recv,
):
    wc = width // CHUNKS
    half = wc // 2
    quarter = wc // 4
    ep = lax.axis_index("ep")
    fs = lax.axis_index("fs")
    y, core = ep // 2, ep % 2
    z, x = fs // 4, fs % 4

    def on_y(step):
        return {"ep": ((y + step) % 4) * 2 + core}

    def on_x(step):
        return {"fs": z * 4 + (x + step) % 4}

    def on_z(step):
        return {"fs": ((z + step) % 4) * 4 + x}

    partner = {"ep": y * 2 + (1 - core)}

    def await_bytes(sem, rows, size):
        where = grads.at[pl.ds(0, rows // ROWS), :, pl.ds(0, size)]
        pltpu.make_async_copy(where, where, sem).wait()


    def cols(k, start=0, size=None):
        return pl.ds(pl.multiple_of(k * wc + start, LANE), wc if size is None else size)

    def grads_load(n):
        pair = pl.ds(((y + STEPS[n]) % 4) * 2, 2)
        return pltpu.make_async_copy(grads_hbm.at[0, pair], grads.at[pair], load_sem.at[n])

    state_loads = [
        pltpu.make_async_copy(src.at[0], dst, load_sem.at[4])
        for src, dst in ((weight_hbm, weight), (mom_hbm, mom), (second_hbm, second))
    ]
    barrier = pltpu.get_barrier_semaphore()
    peers = [partner, on_y(1), on_y(3)]
    peers += [{"fs": ((z + dz) % 4) * 4 + (x + dx) % 4} for dx, dz in OTHERS]
    for peer in peers:
        pl.semaphore_signal(barrier, inc=1, device_id=peer, device_id_type=MESH)

    small_loads = [
        pltpu.make_async_copy(src, dst, load_sem.at[5 + i])
        for i, (src, dst) in enumerate(
            (
                (counts_hbm, counts),
                (in_weight_hbm, in_weight),
                (in_bias_hbm, in_bias),
                (out_weight_hbm, out_weight),
                (out_bias_hbm, out_bias),
            )
        )
    ]
    small_loads[0].start()
    for n in range(4):
        grads_load(n).start()

    small_loads[0].wait()
    counted = counts[...].astype(F32)
    share_table = counted / jnp.sum(counted, axis=0, keepdims=True)
    row_id = lax.broadcasted_iota(jnp.int32, (8, 8), 0)
    col_id = lax.broadcasted_iota(jnp.int32, (8, 8), 1)
    for i in range(8):
        c = core if i >= 4 else 1 - core
        e = ((y + STEPS[i % 4]) % 4) * 2 + c
        picked = jnp.where((row_id == ep) & (col_id == e), share_table, 0.0)
        one = jnp.sum(jnp.sum(picked, axis=1, keepdims=True), axis=0, keepdims=True)
        shares[i] = jnp.broadcast_to(one, (ROWS, LANE))

    with jax.named_scope("barrier"):
        pl.semaphore_wait(barrier, len(peers))

    tiles = wc // LANE
    half_tiles = half // LANE

    def tile(k, t):
        return pl.ds(pl.multiple_of(k * wc + t * LANE, LANE), LANE)

    def pair_copy(part, k):
        which = pl.ds(0, 1) if part == 0 else pl.ds(1, 3)
        return pltpu.make_async_remote_copy(
            src_ref=to_pair.at[which, :, cols(k)],
            dst_ref=from_pair.at[which, :, cols(k)],
            send_sem=early_send.at[0],
            recv_sem=pair_recv.at[part, k],
            device_id=partner,
            device_id_type=MESH,
        )

    def weigh(part, k):
        def body(t):
            at = tile(k, t)
            for n in (0,) if part == 0 else (1, 2, 3):
                e = ((y + STEPS[n]) % 4) * 2 + (1 - core)
                to_pair[n, :, at] = (grads[e, :, at].astype(F32) * shares[n]).astype(BF16)

        loop(tiles, body, unroll=4)
        pair_copy(part, k).start()

    with jax.named_scope("weigh"):
        grads_load(0).wait()
        loop(CHUNKS, functools.partial(weigh, 0))
        for n in (1, 2, 3):
            grads_load(n).wait()
        loop(HEAD, functools.partial(weigh, 1))

    def ring_copy(src, dst, kind, k, start, size, device):
        return pltpu.make_async_remote_copy(
            src_ref=src.at[:, cols(k, start, size)],
            dst_ref=dst.at[:, cols(k, start, size)],
            send_sem=early_send.at[0],
            recv_sem=ring_recv.at[kind // 2 if kind < 2 else 1, k],
            device_id=device,
            device_id_type=MESH,
        )

    def far_a(k):
        return ring_copy(far_out, far_in, 0, k, 0, half, on_y(1))

    def far_b(k):
        return ring_copy(far_out, far_in, 1, k, half, half, on_y(3))

    def up_a(k):
        return ring_copy(up_out, up_in, 2, k, 0, half, on_y(1))

    def up_b(k):
        return ring_copy(up_out, up_in, 3, k, half, half, on_y(1))

    def down_a(k):
        return ring_copy(down_out, down_in, 4, k, 0, half, on_y(3))

    def down_b(k):
        return ring_copy(down_out, down_in, 5, k, half, half, on_y(3))

    def pair_sum(step, at):
        n = STEPS.index(step)
        e = ((y + step) % 4) * 2 + core
        mine = (grads[e, :, at].astype(F32) * shares[4 + n]).astype(BF16).astype(F32)
        return mine + from_pair[n, :, at].astype(F32)

    def sum_far(k):
        pair_copy(0, k).wait_recv()

        def far(t):
            at = tile(k, t)
            far_out[:, at] = encode(pair_sum(2, at))

        loop(tiles, far, unroll=2)
        far_a(k).start()
        far_b(k).start()

    def sum_near(k):
        pair_copy(1, k).wait_recv()

        def first(t):
            a, b = tile(k, t), tile(k, t + half_tiles)
            down_out[:, a] = encode(pair_sum(3, a))
            up_out[:, b] = encode(pair_sum(1, b))

        loop(half_tiles, first, unroll=2)
        up_b(k).start()
        down_a(k).start()

        def rest(t):
            a, b = tile(k, t), tile(k, t + half_tiles)
            part_sum[:, a] = pair_sum(1, a)
            part_sum[:, b] = pair_sum(3, b)
            own_sum[:, a] = pair_sum(0, a)
            own_sum[:, b] = pair_sum(0, b)

        loop(half_tiles, rest, unroll=2)

    with jax.named_scope("sum_pairs"):
        @pl.when(core == FIRST_CORE)
        def _():
            loop(CHUNKS, sum_far)

        for load in small_loads[1:] + state_loads:
            load.start()
        loop(CHUNKS - HEAD, lambda k: weigh(1, HEAD + k))

        @pl.when(core != FIRST_CORE)
        def _():
            pl.semaphore_wait(go, 1)
            loop(CHUNKS, sum_far)

        loop(CHUNKS, sum_near)

    for load in small_loads[1:]:
        load.wait()
    wide = (ROWS, LANE)
    lane = lax.broadcasted_iota(jnp.int32, wide, 1)
    same_row = lane % 8 == lax.broadcasted_iota(jnp.int32, wide, 0) % 8
    first_unit = lax.broadcasted_iota(jnp.int32, wide, 0) < 8
    feature = jnp.where(lane < 96, (lane % 32) // 8, jnp.where(lane < 120, 4, 5))
    low = (lane >= 112) & (lane < 120)
    mid = (lane // 32 == 1) | ((lane >= 104) & (lane < 112))

    def unit_rows(jj):
        return pl.ds(pl.multiple_of(16 * jj, 16), 16)

    def fill_base(jj):
        value = jnp.zeros(wide, F32)
        for i in range(5):
            pair = jnp.where(first_unit, in_weight[i, 2 * jj], in_weight[i, 2 * jj + 1])
            value = jnp.where((feature == i) & same_row, pair, value)
        base[unit_rows(jj), :] = value
        for j in (2 * jj, 2 * jj + 1):
            for i in range(2):
                table[j, i] = jnp.full((8, LANE), out_weight[i, j], F32)

    with jax.named_scope("fill"):
        loop(16, fill_base)

    def pass_on(k):
        @pl.when((core == FIRST_CORE) & (k == GO_CHUNK))
        def _():
            pl.semaphore_signal(go, inc=1, device_id=partner, device_id_type=MESH)

        await_bytes(ring_recv.at[0, k], ROWS, wc)

        def up(t):
            at = tile(k, t)
            up_out[:, at] = encode(part_sum[:, at] + decode(far_in[:, at]))

        loop(half_tiles, up, unroll=2)
        up_a(k).start()

        def down(t):
            at = tile(k, t + half_tiles)
            down_out[:, at] = encode(part_sum[:, at] + decode(far_in[:, at]))

        loop(half_tiles, down, unroll=2)
        down_b(k).start()

    with jax.named_scope("pass_on"):
        loop(CHUNKS, pass_on)

    await_bytes(load_sem.at[4], 5 * ROWS, width)

    def moments(k, sums):
        await_bytes(ring_recv.at[1, k], 2 * ROWS, wc)

        def body(t, sums):
            grad_sq, mom_sq = sums
            at = tile(k, t)
            gradient = own_sum[:, at] + decode(up_in[:, at]) + decode(down_in[:, at])
            mom_next = MOMENTUM_DECAY * mom[:, at] + (1.0 - MOMENTUM_DECAY) * gradient
            squared = gradient * gradient
            own_sum[:, at] = gradient
            new_mom[:, at] = mom_next
            new_second[:, at] = SECOND_DECAY * second[:, at] + (1.0 - SECOND_DECAY) * squared
            return grad_sq + squared, mom_sq + mom_next * mom_next

        return lax.fori_loop(0, tiles, body, sums, unroll=2)

    zero = jnp.zeros((ROWS, LANE), F32)
    with jax.named_scope("moments"):
        grad_sq, mom_sq = lax.fori_loop(0, CHUNKS, moments, (zero, zero))

    sums_out[...] = jnp.concatenate(
        [jnp.sum(grad_sq, axis=0, keepdims=True), jnp.sum(mom_sq, axis=0, keepdims=True)], axis=0
    )
    sums_in[fs] = sums_out[...]

    def sums_copy(dx, dz):
        return pltpu.make_async_remote_copy(
            src_ref=sums_out,
            dst_ref=sums_in.at[fs],
            send_sem=sums_sem.at[0],
            recv_sem=sums_sem.at[1],
            device_id={"fs": ((z + dz) % 4) * 4 + (x + dx) % 4},
            device_id_type=MESH,
        )

    for dx, dz in OTHERS:
        sums_copy(dx, dz).start()
    fifteen = sums_in.at[pl.ds(0, 15)]
    last_pair = width // (2 * LANE) - 1
    ones = jnp.ones((8, 2 * LANE), F32)

    def pair_at(p):
        return pl.ds(pl.multiple_of(p * (2 * LANE), 2 * LANE), 2 * LANE)

    def prepare(p):
        at = pair_at(p)
        w16 = weight[:, at].astype(F32)
        for n in range(2):
            rows = slice(8 * n, 8 * n + 8)
            g = own_sum[rows, at]
            m = new_mom[rows, at]
            w = w16[rows]
            inv_root = lax.rsqrt(new_second[rows, at] + ROOT_EPS)
            a1, b1, _ = pieces(jnp.concatenate([g, m], axis=0))
            a2, b2, _ = pieces(jnp.concatenate([m * inv_root, g * inv_root], axis=0))
            ww = jnp.concatenate([w, w], axis=0)
            wo = jnp.concatenate([w, ones], axis=0)
            for i, part in enumerate((a1, a2, b1, b2, ww, wo)):
                right[p, n, 16 * i : 16 * i + 16, :] = part.astype(BF16)

    with jax.named_scope("prepare"):
        loop(last_pair + 1, prepare)
    with jax.named_scope("sums"):
        pltpu.make_async_copy(fifteen, fifteen, sums_sem.at[1]).wait()
    total = sums_in[0]
    for i in range(1, 16):
        total = total + sums_in[i]

    entries = float(ROWS * width * 16)
    total = jnp.sum(total, axis=1, keepdims=True)
    grad_var = total[0:1] / entries + NORM_EPS
    mom_var = total[1:2] / entries + NORM_EPS
    inv_grad = jnp.broadcast_to(lax.rsqrt(grad_var), wide)
    inv_mom = jnp.broadcast_to(lax.rsqrt(mom_var), wide)
    log_mom = jnp.broadcast_to(0.5 * jnp.log(mom_var), (ROWS, LANE))

    scale = jnp.where(feature == 0, inv_grad, jnp.where(feature == 1, inv_mom, 1.0))

    def fill_matrix(jj):
        a, b, c = pieces(base[unit_rows(jj), :] * scale)
        value = jnp.where(low, c, jnp.where(mid, b, a))
        slope = jnp.where(first_unit, in_weight[5, 2 * jj], in_weight[5, 2 * jj + 1])
        shift = jnp.where(first_unit, in_bias[2 * jj], in_bias[2 * jj + 1])
        a, b, c = pieces(log_mom * slope + shift)
        bias = jnp.where(lane == 120, a, jnp.where(lane == 121, b, c))
        bias = jnp.where((lane >= 120) & (lane < 123), bias, 0.0)
        matrix[unit_rows(jj), :] = (value + bias).astype(BF16)

    with jax.named_scope("matrix"):
        loop(16, fill_matrix, unroll=2)
    direction_bias = jnp.full((8, LANE), out_bias[0], F32)
    magnitude_bias = jnp.full((8, LANE), out_bias[1], F32)


    def first_layer(p, hidden):
        p = jnp.minimum(p, last_pair)
        for n in range(2):
            parts = [right[p, n, 16 * i : 16 * i + 16, :] for i in range(6)]
            order = (0, 1, 0, 1, 2, 3, 4, 5)
            whole = jnp.concatenate([parts[i] for i in order], axis=0)
            hidden[n] = jnp.dot(matrix[...], whole, preferred_element_type=F32)

    def second_layer(p, hidden):
        at = pair_at(p)
        direction = [direction_bias] * 4
        magnitude = [magnitude_bias] * 4
        for j in range(32):
            to_direction, to_magnitude = table[j, 0], table[j, 1]
            for v in range(4):
                n, half_at = v // 2, v % 2
                h = hidden[n, 8 * j : 8 * j + 8, LANE * half_at : LANE * (half_at + 1)]
                h = jnp.maximum(h, 0.0)
                direction[v] = direction[v] + to_direction * h
                magnitude[v] = magnitude[v] + to_magnitude * h
        update = [
            STEP_SCALE * direction[v] * jnp.exp(EXP_SCALE * magnitude[v]) for v in range(4)
        ]
        rows = [jnp.concatenate(update[2 * n : 2 * n + 2], axis=1) for n in range(2)]
        fresh = weight[:, at].astype(F32) - jnp.concatenate(rows, axis=0)
        gathered[z, x, :, at] = fresh.astype(BF16)

    pairs = tiles // 2

    def network(k):
        def body(t):
            p = k * pairs + 2 * t
            first_layer(p + 1, hidden_b)
            second_layer(p, hidden_a)
            first_layer(p + 2, hidden_a)
            second_layer(p + 1, hidden_b)

        loop(pairs // 2, body)

    first_layer(0, hidden_a)

    ONE, TWO, THEN = 0, 1, 2
    LAST = None
    FULL, H1, H2 = (0, wc), (0, half), (half, half)
    B1, A1, A2, B2 = ((i * quarter, quarter) for i in range(4))

    def push(dx, dz, k, part, device, sem):
        at = cols(k, *part)
        if dx is None:
            where = gathered.at[(z + dz) % 4, :, :, at]
        elif dz is None:
            where = gathered.at[:, (x + dx) % 4, :, at]
        else:
            where = gathered.at[(z + dz) % 4, (x + dx) % 4, :, at]
        pltpu.make_async_remote_copy(
            src_ref=where,
            dst_ref=where,
            send_sem=gather_send.at[1 if part == FULL or sem == TWO or 2 in (dx, dz) else 0],
            recv_sem=last_recv.at[0] if sem is LAST else gather_recv.at[sem, k],
            device_id=device,
            device_id_type=MESH,
        ).start()

    def arrived(sem, k, blocks=1):
        await_bytes(gather_recv.at[sem, k], blocks * ROWS, wc)

    def send_own(k):
        for toward in (1, 3):
            push(0, 0, k, FULL, on_x(toward), ONE)
            push(0, 0, k, FULL, on_z(toward), ONE)

    def along_z(dx, dz, k):
        push(dx, dz, k, H1, on_z(1), THEN)
        push(dx, dz, k, H1, on_z(3), THEN)

    def along_x(dx, dz, k):
        push(dx, dz, k, H2, on_x(1), THEN)
        push(dx, dz, k, H2, on_x(3), THEN)

    def relay_near(k):
        arrived(ONE, k, 4)
        push(3, 0, k, A1, on_x(1), TWO)
        push(1, 0, k, B1, on_x(3), TWO)
        push(0, 3, k, A2, on_z(1), TWO)
        push(0, 1, k, B2, on_z(3), TWO)
        for d in (3, 1):
            along_z(d, 0, k)
            along_x(0, d, k)

    def relay_far(k):
        arrived(TWO, k)
        along_z(2, 0, k)
        along_x(0, 2, k)

    def relay_last(k):
        arrived(THEN, k, 6)
        push(None, 3, k, A1, on_z(1), LAST)
        push(None, 1, k, B1, on_z(3), LAST)
        push(3, None, k, A2, on_x(1), LAST)
        push(1, None, k, B2, on_x(3), LAST)

    def step(t):
        @pl.when(t < CHUNKS)
        def _():
            with jax.named_scope("network"):
                network(t)
            send_own(t)

        for lag, relay in zip(LAG, (relay_near, relay_far, relay_last)):

            @pl.when((t >= lag) & (t < CHUNKS + lag))
            def _(lag=lag, relay=relay):
                relay(t - lag)

    with jax.named_scope("gather"):
        loop(CHUNKS + LAG[-1], step)

    with jax.named_scope("drain"):
        await_bytes(last_recv.at[0], 4 * ROWS, width)
    await_bytes(early_send.at[0], 7 * ROWS, width)
    pltpu.make_async_copy(fifteen, fifteen, sums_sem.at[0]).wait()
    with jax.named_scope("final"):
        await_bytes(gather_send.at[0], 8 * ROWS, width)
        await_bytes(gather_send.at[1], 7 * ROWS, width)


def pieces(x):
    a = x.astype(BF16).astype(F32)
    b = (x - a).astype(BF16).astype(F32)
    return a, b, x - a - b


def write_out(gathered, new_mom, new_second, gathered_hbm, mom_hbm, second_hbm, sem):
    copies = [
        pltpu.make_async_copy(
            gathered.at[i // 4, i % 4], gathered_hbm.at[0, pl.ds(i * ROWS, ROWS)], sem.at[i]
        )
        for i in range(16)
    ]
    copies.append(pltpu.make_async_copy(new_mom, mom_hbm.at[0], sem.at[16]))
    copies.append(pltpu.make_async_copy(new_second, second_hbm.at[0], sem.at[17]))
    for copy in copies:
        copy.start()
    for copy in copies:
        copy.wait()


def per_device(grads, counts, weight, mom, second, in_weight, in_bias, out_weight, out_bias):
    rows, width = mom.shape[1:]
    hbm = pl.BlockSpec(memory_space=pltpu.HBM)
    vmem = pl.BlockSpec(memory_space=pltpu.VMEM)
    dma = pltpu.SemaphoreType.DMA
    gathered, new_mom, new_second = pl.pallas_call(
        functools.partial(kernel, width),
        out_shape=(
            pltpu.VMEM((4, 4, rows, width), BF16),
            pltpu.VMEM((rows, width), F32),
            pltpu.VMEM((rows, width), F32),
        ),
        in_specs=[hbm] * 9,
        out_specs=(vmem, vmem, vmem),
        scratch_shapes=[
            pltpu.VMEM((8, 8), jnp.int32),
            pltpu.SMEM((6, 32), F32),
            pltpu.SMEM((32,), F32),
            pltpu.SMEM((2, 32), F32),
            pltpu.SMEM((2,), F32),
            pltpu.VMEM((8, rows, width), BF16),
            pltpu.VMEM((rows, width), BF16),
            pltpu.VMEM((rows, width), F32),
            pltpu.VMEM((rows, width), F32),
            pltpu.VMEM((4, rows, width), BF16),
            pltpu.VMEM((4, rows, width), BF16),
            *[pltpu.VMEM((rows, width), BF16)] * 6,
            pltpu.VMEM((rows, width), F32),
            pltpu.VMEM((rows, width), F32),
            pltpu.VMEM((8, rows, LANE), F32),
            pltpu.VMEM((32, 2, 8, LANE), F32),
            pltpu.VMEM((256, LANE), BF16),
            pltpu.VMEM((256, LANE), F32),
            pltpu.VMEM((width // 256, 2, 96, 256), BF16),
            pltpu.VMEM((2, 256, 256), F32),
            pltpu.VMEM((2, 256, 256), F32),
            pltpu.VMEM((2, LANE), F32),
            pltpu.VMEM((16, 2, LANE), F32),
            dma((10,)),
            pltpu.SemaphoreType.REGULAR,
            dma((1,)),
            dma((2, CHUNKS)),
            dma((2, CHUNKS)),
            dma((2,)),
            dma((2,)),
            dma((3, CHUNKS)),
            dma((1,)),
        ],
        compiler_params=pltpu.CompilerParams(
            collective_id=0, has_side_effects=True, vmem_limit_bytes=36 << 20
        ),
        name="learned_step",
    )(*[
        pltpu.with_memory_space_constraint(a, pltpu.HBM)
        for a in (counts, in_weight, in_bias, out_weight.T, out_bias, grads, weight, mom, second)
    ])
    return pl.pallas_call(
        write_out,
        out_shape=tuple(
            jax.ShapeDtypeStruct(shape, dtype)
            for shape, dtype in (
                ((1, 16 * rows, width), BF16),
                ((1, rows, width), F32),
                ((1, rows, width), F32),
            )
        ),
        in_specs=[vmem] * 3,
        out_specs=(hbm,) * 3,
        scratch_shapes=[dma((18,))],
        compiler_params=pltpu.CompilerParams(vmem_limit_bytes=1 << 20),
        name="write_out",
    )(gathered, new_mom, new_second)


def solution(mesh):
    in_specs = (
        P("ep", None, "fs", None),
        P(),
        P("ep", "fs", None),
        P("ep", "fs", None),
        P("ep", "fs", None),
        P(),
        P(),
        P(),
        P(),
    )
    out_specs = (P("ep", None, None), P("ep", "fs", None), P("ep", "fs", None))
    return jax.shard_map(
        per_device, mesh=mesh, in_specs=in_specs, out_specs=out_specs, check_vma=False
    )
```
